128 devices in a mesh: batch: 1, ctx: 64 (over z, y, x), seq: 2 (over core).
Axes of the slice: x: 4, y: 4, z: 4, core: 2. Of those that a mesh axis runs over, the one named last changes fastest.
Arguments:
- hidden: bfloat16 [16, 5120], P('batch')
- lengths: int32 [16], P('batch')
- latent_cache: bfloat16 [16, 8192, 512], P('batch', ('ctx', 'seq'))
- rope_keys: bfloat16 [16, 8192, 64], P('batch', ('ctx', 'seq'))
- w_uq: bfloat16 [5120, 128, 128], P(None, 'seq')
- w_qr: bfloat16 [5120, 128, 64], P(None, 'seq')
- w_uk: bfloat16 [128, 128, 512], P('seq')
- w_uv: bfloat16 [128, 512, 128], P('seq')
- w_out: bfloat16 [128, 128, 5120], P('seq')
Outputs:
- output: bfloat16 [16, 5120], P('batch')
All inputs are finite; a program needn't handle non-finite values.
Results may differ from the reference program's by a relative error of at most 0.00571221.
Values are sent between devices in bfloat16 or wider.
A program may use at most 1 GiB of HBM per device.

```python
import jax
import jax.numpy as jnp
from jax import lax

NUM_ROWS = 16
SEQ_LEN = 8192
D_MODEL = 5120
NUM_HEADS = 128
LATENT = 512
ROPE_DIM = 64
NOPE_DIM = 128
VALUE_DIM = 128
NUM_WAVES = 3

SCORE_SCALE = (NOPE_DIM + ROPE_DIM) ** -0.5
SHORT_LEN = SEQ_LEN // 8
LONG_LEN = SEQ_LEN - SEQ_LEN // 8


def wave_basis():
    spots = (jnp.arange(SEQ_LEN, dtype=jnp.float32) + 0.5) / SEQ_LEN
    waves = jnp.arange(1, NUM_WAVES + 1, dtype=jnp.float32)
    return jnp.cos(jnp.pi * spots[:, None] * waves[None, :])


def draw_rows(row_keys, width, amplitude, profile):
    def one_row(row_key):
        coef_key, noise_key = jax.random.split(row_key)
        coeffs = amplitude * jax.random.normal(coef_key, (NUM_WAVES, width), jnp.float32)
        noise = jax.random.normal(noise_key, (SEQ_LEN, width), jnp.float32)
        return (0.6 * noise + jnp.dot(profile, coeffs)).astype(jnp.bfloat16)
    return lax.map(one_row, row_keys)


def draw_lengths(len_key):
    coin_key, long_key, short_key = jax.random.split(len_key, 3)
    coins = jax.random.randint(coin_key, (NUM_ROWS,), 0, 2)
    long_lens = jax.random.randint(long_key, (NUM_ROWS,), LONG_LEN, SEQ_LEN + 1)
    short_lens = jax.random.randint(short_key, (NUM_ROWS,), SHORT_LEN, SEQ_LEN + 1)
    lengths = jnp.where(coins == 1, long_lens, short_lens)
    return lengths.at[0].set(SEQ_LEN).at[1].set(SHORT_LEN).astype(jnp.int32)


def setup_inputs(seed: int = 0, part: int = 0) -> dict:
    base_key = jax.random.key(seed)
    part_key = jax.random.fold_in(base_key, part)
    weight_keys = jax.random.split(base_key, 5)
    data_keys = jax.random.split(part_key, 4)
    profile = wave_basis()
    q_scale = 0.6 * D_MODEL ** -0.5
    hidden = jax.random.normal(data_keys[0], (NUM_ROWS, D_MODEL), jnp.float32)
    w_uq = q_scale * jax.random.normal(weight_keys[0], (D_MODEL, NUM_HEADS, NOPE_DIM), jnp.float32)
    w_qr = q_scale * jax.random.normal(weight_keys[1], (D_MODEL, NUM_HEADS, ROPE_DIM), jnp.float32)
    w_uk = NOPE_DIM ** -0.5 * jax.random.normal(weight_keys[2], (NUM_HEADS, NOPE_DIM, LATENT), jnp.float32)
    w_uv = LATENT ** -0.5 * jax.random.normal(weight_keys[3], (NUM_HEADS, LATENT, VALUE_DIM), jnp.float32)
    w_out = (NUM_HEADS * VALUE_DIM) ** -0.5 * jax.random.normal(weight_keys[4], (NUM_HEADS, VALUE_DIM, D_MODEL), jnp.float32)
    return {
        'hidden': hidden.astype(jnp.bfloat16),
        'lengths': draw_lengths(data_keys[1]),
        'latent_cache': draw_rows(jax.random.split(data_keys[2], NUM_ROWS), LATENT, 1.0, profile),
        'rope_keys': draw_rows(jax.random.split(data_keys[3], NUM_ROWS), ROPE_DIM, 2.0, profile),
        'w_uq': w_uq.astype(jnp.bfloat16),
        'w_qr': w_qr.astype(jnp.bfloat16),
        'w_uk': w_uk.astype(jnp.bfloat16),
        'w_uv': w_uv.astype(jnp.bfloat16),
        'w_out': w_out.astype(jnp.bfloat16),
    }


def reference(hidden, lengths, latent_cache, rope_keys, w_uq, w_qr, w_uk, w_uv, w_out):
    q_nope = jnp.dot(hidden, w_uq.reshape(D_MODEL, NUM_HEADS * NOPE_DIM), preferred_element_type=jnp.float32)
    q_nope = q_nope.astype(jnp.bfloat16).reshape(NUM_ROWS, NUM_HEADS, NOPE_DIM)
    q_rope = jnp.dot(hidden, w_qr.reshape(D_MODEL, NUM_HEADS * ROPE_DIM), preferred_element_type=jnp.float32)
    q_rope = q_rope.astype(jnp.bfloat16).reshape(NUM_ROWS, NUM_HEADS, ROPE_DIM)
    q_lat = jnp.einsum('bhk,hkc->bhc', q_nope.astype(jnp.float32), w_uk.astype(jnp.float32)).astype(jnp.bfloat16)
    positions = jnp.arange(SEQ_LEN)

    def one_row(row_data):
        lat_row, rope_row, cache_row, keys_row, length = row_data
        scores = jnp.dot(lat_row, cache_row.T, preferred_element_type=jnp.float32)
        scores = (scores + jnp.dot(rope_row, keys_row.T, preferred_element_type=jnp.float32)) * SCORE_SCALE
        valid = positions[None, :] < length
        scores = jnp.where(valid, scores, -jnp.inf)
        row_max = jnp.max(scores, axis=1, keepdims=True)
        weights = jnp.exp(scores - row_max)
        weight_sum = jnp.sum(weights, axis=1, keepdims=True)
        weighted = jnp.dot(weights.astype(jnp.bfloat16), cache_row, preferred_element_type=jnp.float32)
        return (weighted / weight_sum).astype(jnp.bfloat16)

    lat_out = lax.map(one_row, (q_lat, q_rope, latent_cache, rope_keys, lengths))
    head_vals = jnp.einsum('bhc,hcv->bhv', lat_out.astype(jnp.float32), w_uv.astype(jnp.float32)).astype(jnp.bfloat16)
    mixed = jnp.einsum('bhv,hvd->bd', head_vals.astype(jnp.float32), w_out.astype(jnp.float32))
    return (hidden.astype(jnp.float32) + mixed).astype(jnp.bfloat16)
```

```python
import functools

import jax
import jax.numpy as jnp
from jax import lax
from jax.experimental import pallas as pl
from jax.experimental.pallas import tpu as pltpu
from jax.sharding import PartitionSpec as P

NEG_FILL = -1.0e30
F32 = jnp.float32
BF16 = jnp.bfloat16

SHIFTS = ((0, 0, 0), (1, 0, 0), (0, 0, -1), (0, 1, 0), (0, -1, 0), (-1, 0, -1), (0, -1, 1), (0, 1, 1))
STEPS = ((0, 0), (1, 0), (3, 0), (1, 1), (3, 1), (2, 0), (0, 1), (2, 1))

NT = (((1,), (1,)), ((), ()))


def chip_at(x, y, z):
    return z * 16 + y * 4 + x


def chip_of(group, colour):
    z = group // 2
    y = 2 * (group % 2) + colour // 4
    x = (colour % 4 + 8 - y - z) % 4
    return chip_at(x, y, z)


def kernel(scale, hidden, lengths, latent, rope, wuq, wqr, wuk, wuv, wout, out,
           len_s, hid_s, wq_s, wq_f, wr_s, wuk_s, wuv_s, wout_s, lat_s, rope_s,
           lat_b, rope_b, qp, rs1, q_send, q_all, s_buf, p_buf, acc_send, o_buf,
           v_send, v_all, v_f, y_part, y_sib, y_send, y_all, piece, out_b,
           load_sem, own_sem, c_send, c_recv, r_send, r_recv, rs_send, rs_recv,
           qd_send, qd_recv, a_send, a_recv, v_ssem, v_rsem, d_send, d_recv, y_ssem, y_rsem,
           o_send, o_recv):
    ctx = lax.axis_index('ctx')
    core = lax.axis_index('seq')
    z, y, x = ctx // 16, (ctx // 4) % 4, ctx % 4
    colour = (x + y + z) % 4 + 4 * (y % 2)
    group = z * 2 + y // 2
    other = 1 - core
    row = 2 * colour + core
    dspan = hid_s.shape[2]
    cols = pl.ds(pl.multiple_of(colour * dspan, 128), dspan)
    heads = pl.ds(pl.multiple_of(group * 8, 8), 8)

    def dev(chip, c):
        return (0, chip, c)

    def remote(src, dst, ssem, rsem, device):
        return pltpu.make_async_remote_copy(src_ref=src, dst_ref=dst, send_sem=ssem, recv_sem=rsem,
                                            device_id=device, device_id_type=pl.DeviceIdType.MESH)

    loads = [
        pltpu.make_async_copy(wuq.at[pl.ds(pl.multiple_of(colour * dspan, 128), dspan), heads, :], wq_s, load_sem.at[0]),
        pltpu.make_async_copy(wqr.at[heads, :, cols], wr_s, load_sem.at[1]),
        pltpu.make_async_copy(hidden.at[:, :, cols], hid_s, load_sem.at[2]),
        pltpu.make_async_copy(latent, lat_s, load_sem.at[3]),
        pltpu.make_async_copy(rope, rope_s, load_sem.at[4]),
        pltpu.make_async_copy(wuk.at[heads], wuk_s, load_sem.at[5]),
        pltpu.make_async_copy(wuv.at[heads], wuv_s, load_sem.at[6]),
        pltpu.make_async_copy(wout.at[heads, :, cols], wout_s, load_sem.at[7]),
        pltpu.make_async_copy(lengths, len_s, load_sem.at[8]),
    ]
    for load in loads:
        load.start()

    barrier = pltpu.get_barrier_semaphore()

    def greet(chip, c):
        pl.semaphore_signal(barrier, inc=1, device_id=dev(chip, c), device_id_type=pl.DeviceIdType.MESH)

    me_class = core * 8 + group
    me_tile = colour * 2 + core
    for i in range(1, 16):
        peer = (me_class + i) % 16
        greet(chip_of(peer % 8, colour), peer // 8)
        peer = (me_tile + i) % 16
        greet(chip_of(group, peer // 2), peer % 2)
    sources = []
    for dx, dy, dz in SHIFTS:
        sources.append(chip_at((x + 4 - dx) % 4, (y + 4 - dy) % 4, (z + 4 - dz) % 4))
    for t in range(1, 8):
        for c in range(2):
            greet(sources[t], c)

    loads[0].wait()
    chunk = 64

    @pl.loop(0, dspan // chunk)
    def _(i):
        rows = wq_s[pl.ds(i * chunk, chunk)].astype(F32).reshape(chunk * 8, 128)
        wq_f[pl.ds(pl.multiple_of(i * chunk * 8, 8), chunk * 8), :] = rows

    loads[1].wait()
    loads[2].wait()
    hid = hid_s[...].astype(F32).reshape(16, dspan).astype(BF16)
    for h in range(8):
        w_h = wq_f[pl.ds(h, dspan, stride=8), :].astype(BF16)
        qp[0, pl.ds(h, 16, stride=8), :] = jnp.dot(hid, w_h, preferred_element_type=F32)
    part_r = lax.dot_general(hid, wr_s[...].reshape(512, dspan), NT, preferred_element_type=F32)
    for pair in range(4):
        both = part_r[:, pair * 128:(pair + 1) * 128]
        qp[1, pl.ds(2 * pair, 16, stride=8), :] = both
        qp[1, pl.ds(2 * pair + 1, 16, stride=8), :] = pltpu.roll(both, 64, 1)

    pl.semaphore_wait(barrier, 44)

    started = []

    def pair_rows(c):
        return pl.ds(pl.multiple_of(c * 16, 16), 16)

    for i in range(1, 8):
        peer = (colour + i) % 8
        copy = remote(qp.at[:, pair_rows(peer), :], rs1.at[colour], rs_send.at[peer], rs_recv.at[colour],
                      dev(chip_of(group, peer), core))
        copy.start()
        started.append(copy)
    rs1[colour] = qp[:, pair_rows(colour), :]

    loads[3].wait()
    loads[4].wait()
    own_l = pltpu.make_async_copy(lat_s.at[row], lat_b.at[core], own_sem.at[0])
    own_r = pltpu.make_async_copy(rope_s.at[row], rope_b.at[core], own_sem.at[1])

    def cache_send(t, c):
        dx, dy, dz = SHIFTS[t]
        chip = chip_at((x + 4 + dx) % 4, (y + 4 + dy) % 4, (z + 4 + dz) % 4)
        target = (colour + STEPS[t][0]) % 4 + 4 * ((colour // 4 + STEPS[t][1]) % 2)
        src_row = 2 * target + c
        slot = 2 * t + core
        index = 2 * t + c
        a = remote(lat_s.at[src_row], lat_b.at[slot], c_send.at[index], c_recv.at[slot], dev(chip, c))
        b = remote(rope_s.at[src_row], rope_b.at[slot], r_send.at[index], r_recv.at[slot], dev(chip, c))
        a.start()
        b.start()
        started.extend((a, b))

    for t in (5, 6, 7, 1, 2, 3, 4):
        for c in range(2):
            cache_send(t, c)
    cache_send(0, other)
    own_l.start()
    own_r.start()

    def arrive(dst, rsem):
        remote(dst, dst, rsem, rsem, dev(ctx, other)).wait_recv()

    for i in range(1, 8):
        peer = (colour + i) % 8
        arrive(rs1.at[peer], rs_recv.at[peer])
    total = rs1[0]
    for i in range(1, 8):
        total = total + rs1[i]
    q_nope = total[0].astype(BF16)
    q_rope = jnp.where(lax.broadcasted_iota(jnp.int32, (16, 128), 1) < 64, total[1], 0.0)
    loads[5].wait()
    row_head = lax.broadcasted_iota(jnp.int32, (16, 512), 0) % 8
    q_lat = jnp.zeros((16, 512), F32)
    for h in range(8):
        res = jnp.dot(q_nope, wuk_s[h], preferred_element_type=F32)
        q_lat = jnp.where(row_head == h, res, q_lat)
    for r in range(2):
        q_send[r, :, 0:512] = q_lat[r * 8:(r + 1) * 8].astype(BF16)
        q_send[r, :, 512:640] = q_rope[r * 8:(r + 1) * 8].astype(BF16)
    for i in range(1, 16):
        peer = (me_class + i) % 16
        copy = remote(q_send.at[peer // 8], q_all.at[me_class], qd_send.at[peer], qd_recv.at[me_class],
                      dev(chip_of(peer % 8, colour), peer // 8))
        copy.start()
        started.append(copy)
    q_all[me_class] = q_send[core]

    loads[8].wait()
    length = len_s[row]
    for i in range(1, 16):
        peer = (me_class + i) % 16
        arrive(q_all.at[peer], qd_recv.at[peer])
    own_l.wait()
    own_r.wait()
    queries = q_all[...].astype(F32).reshape(128, 640).astype(BF16)
    lane = lax.broadcasted_iota(jnp.int32, (128, 128), 1)
    arrive(lat_b.at[other], c_recv.at[other])
    arrive(rope_b.at[other], r_recv.at[other])
    top = None
    for t in range(8):
        if t:
            for c in range(2):
                arrive(lat_b.at[2 * t + c], c_recv.at[2 * t + c])
                arrive(rope_b.at[2 * t + c], r_recv.at[2 * t + c])
        keys = lat_b[2 * t:2 * t + 2].reshape(128, 512)
        rkeys = rope_b[2 * t:2 * t + 2].reshape(128, 64)
        s = lax.dot_general(queries[:, 0:512], keys, NT, preferred_element_type=F32)
        s = (s + lax.dot_general(queries[:, 512:576], rkeys, NT, preferred_element_type=F32)) * scale
        s = jnp.where(sources[t] * 128 + lane < length, s, NEG_FILL)
        s_buf[:, t * 128:(t + 1) * 128] = s
        m_t = jnp.max(s, axis=1, keepdims=True)
        top = m_t if top is None else jnp.maximum(top, m_t)
    den = jnp.zeros((128, 1), F32)
    for t in range(8):
        valid = sources[t] * 128 + lane < length
        w = jnp.where(valid, jnp.exp(s_buf[:, t * 128:(t + 1) * 128] - top), 0.0)
        den = den + jnp.sum(w, axis=1, keepdims=True)
        p_buf[:, t * 128:(t + 1) * 128] = w.astype(BF16)
    acc = jnp.dot(p_buf[...], lat_b[...].reshape(1024, 512), preferred_element_type=F32)
    acc_send[:, :, 0:512] = acc.reshape(16, 8, 512)
    acc_send[:, :, 512:640] = jnp.where(lane == 0, top, den).reshape(16, 8, 128)

    for i in range(1, 16):
        peer = (me_class + i) % 16
        copy = remote(acc_send.at[peer], o_buf.at[me_class], a_send.at[peer], a_recv.at[me_class],
                      dev(chip_of(peer % 8, colour), peer // 8))
        copy.start()
        started.append(copy)
    o_buf[me_class] = acc_send[me_class]
    for i in range(1, 16):
        peer = (me_class + i) % 16
        arrive(o_buf.at[peer], a_recv.at[peer])
    finished = []
    for r in range(2):
        m_all = [o_buf[r * 8 + g, :, 512:513] for g in range(8)]
        best = functools.reduce(jnp.maximum, m_all)
        num = jnp.zeros((8, 512), F32)
        den_r = jnp.zeros((8, 1), F32)
        for g in range(8):
            factor = jnp.exp(m_all[g] - best)
            num = num + o_buf[r * 8 + g, :, 0:512] * factor
            den_r = den_r + o_buf[r * 8 + g, :, 513:514] * factor
        finished.append(num / den_r)
    o_lat = jnp.concatenate(finished, axis=0).astype(BF16)
    loads[6].wait()
    row_head = lax.broadcasted_iota(jnp.int32, (16, 128), 0) % 8
    vals = jnp.zeros((16, 128), F32)
    for h in range(8):
        res = jnp.dot(o_lat, wuv_s[h], preferred_element_type=F32)
        vals = jnp.where(row_head == h, res, vals)
    v_send[...] = vals.astype(BF16)
    for i in range(1, 8):
        peer = (colour + i) % 8
        copy = remote(v_send, v_all.at[colour], v_ssem.at[peer], v_rsem.at[colour], dev(chip_of(group, peer), core))
        copy.start()
        started.append(copy)
    v_all[colour] = v_send[...]
    for i in range(1, 8):
        peer = (colour + i) % 8
        arrive(v_all.at[peer], v_rsem.at[peer])

    v_f[...] = v_all[...].astype(F32).reshape(128, 128)
    loads[7].wait()
    mixed = jnp.zeros((16, dspan), F32)
    for h in range(8):
        v_h = v_f[pl.ds(h, 16, stride=8), :].astype(BF16)
        mixed = mixed + jnp.dot(v_h, wout_s[h], preferred_element_type=F32)
    y_part[...] = mixed.reshape(2, 8, dspan)
    swap = remote(y_part.at[other], y_sib, d_send, d_recv, dev(ctx, other))
    swap.start()
    swap.wait_recv()
    y_send[...] = y_part[core] + y_sib[...]
    for i in range(1, 8):
        peer = (group + i) % 8
        copy = remote(y_send, y_all.at[group], y_ssem.at[peer], y_rsem.at[group], dev(chip_of(peer, colour), core))
        copy.start()
        started.append(copy)
    y_all[group] = y_send[...]
    for i in range(1, 8):
        peer = (group + i) % 8
        arrive(y_all.at[peer], y_rsem.at[peer])
    y_sum = y_all[0]
    for g in range(1, 8):
        y_sum = y_sum + y_all[g]
    piece[...] = (hid_s[core].astype(F32) + y_sum).astype(BF16)
    for i in range(1, 16):
        peer = (me_tile + i) % 16
        copy = remote(piece, out_b.at[me_tile], o_send.at[peer], o_recv.at[me_tile],
                      dev(chip_of(group, peer // 2), peer % 2))
        copy.start()
        started.append(copy)
    out_b[me_tile] = piece[...]
    for i in range(1, 16):
        peer = (me_tile + i) % 16
        arrive(out_b.at[peer], o_recv.at[peer])
    for slot in range(16):
        out[slot % 2, :, (slot // 2) * dspan:(slot // 2 + 1) * dspan] = out_b[slot]
    swap.wait_send()
    for copy in started:
        copy.wait_send()


def solution(mesh):
    row_spec = P('batch', None)
    cache_spec = P('batch', ('ctx', 'seq'), None)
    proj_spec = P(None, 'seq', None)
    head_spec = P('seq', None, None)

    def local_step(hidden, lengths, latent_cache, rope_keys, w_uq, w_qr, w_uk, w_uv, w_out):
        scale = (w_uq.shape[2] + w_qr.shape[2]) ** -0.5
        width = hidden.shape[1]
        dspan = width // 8
        vmem, dma = pltpu.VMEM, pltpu.SemaphoreType.DMA
        anywhere = pl.BlockSpec(memory_space=pl.ANY)
        scratch = [
            pltpu.SMEM((16,), jnp.int32),
            vmem((2, 8, dspan), BF16),
            vmem((dspan, 8, 128), BF16),
            vmem((dspan * 8, 128), F32),
            vmem((8, 64, dspan), BF16),
            vmem((8, 128, 512), BF16),
            vmem((8, 512, 128), BF16),
            vmem((8, 128, dspan), BF16),
            vmem((16, 64, 512), BF16),
            vmem((16, 64, 64), BF16),
            vmem((16, 64, 512), BF16),
            vmem((16, 64, 64), BF16),
            vmem((2, 128, 128), F32),
            vmem((8, 2, 16, 128), F32),
            vmem((2, 8, 640), BF16),
            vmem((16, 8, 640), BF16),
            vmem((128, 1024), F32),
            vmem((128, 1024), BF16),
            vmem((16, 8, 640), F32),
            vmem((16, 8, 640), F32),
            vmem((16, 128), BF16),
            vmem((8, 16, 128), BF16),
            vmem((128, 128), F32),
            vmem((2, 8, dspan), F32),
            vmem((8, dspan), F32),
            vmem((8, dspan), F32),
            vmem((8, 8, dspan), F32),
            vmem((8, dspan), BF16),
            vmem((16, 8, dspan), BF16),
            dma((9,)), dma((2,)), dma((16,)), dma((16,)), dma((16,)), dma((16,)), dma((8,)), dma((8,)),
            dma((16,)), dma((16,)), dma((16,)), dma((16,)), dma((8,)), dma((8,)), dma, dma, dma((8,)), dma((8,)),
            dma((16,)), dma((16,)),
        ]
        out = pl.pallas_call(
            functools.partial(kernel, scale),
            out_shape=jax.ShapeDtypeStruct((2, 8, width), BF16),
            in_specs=[anywhere] * 9,
            out_specs=pl.BlockSpec(memory_space=pltpu.VMEM),
            scratch_shapes=scratch,
            compiler_params=pltpu.CompilerParams(collective_id=0, has_side_effects=True,
                                                 vmem_limit_bytes=67043328),
            name='mla_decode',
        )(hidden.reshape(2, 8, width), lengths, latent_cache, rope_keys, w_uq,
          jnp.transpose(w_qr, (1, 2, 0)), w_uk, w_uv, w_out)
        return out.reshape(16, width)

    return jax.shard_map(local_step, mesh=mesh,
                         in_specs=(row_spec, P('batch'), cache_spec, cache_spec, proj_spec, proj_spec, head_spec, head_spec, head_spec),
                         out_specs=row_spec, check_vma=False)
```

```python
import functools

import jax
import jax.numpy as jnp
from jax import lax
from jax.experimental import pallas as pl
from jax.experimental.pallas import tpu as pltpu
from jax.sharding import PartitionSpec as P

NEG_FILL = -1.0e30
F32 = jnp.float32
BF16 = jnp.bfloat16

SHIFTS = ((0, 0, 0), (1, 0, 0), (0, 0, -1), (0, 1, 0), (0, -1, 0), (-1, 0, -1), (1, -1, 0), (0, 1, 1))
STEPS = ((0, 0), (1, 0), (3, 0), (1, 1), (3, 1), (2, 0), (0, 1), (2, 1))

NT = (((1,), (1,)), ((), ()))


def chip_at(x, y, z):
    return z * 16 + y * 4 + x


def chip_of(group, colour):
    z = group // 2
    y = 2 * (group % 2) + colour // 4
    x = (colour % 4 + 8 - y - z) % 4
    return chip_at(x, y, z)


def kernel(scale, hidden, lengths, latent, rope, wuq, wqr, wuk, wuv, wout, out,
           len_s, hid_s, hid_r, wq_s, wq_f, wr_s, wuk_s, wuv_s, wout_s, lat_s, rope_s, rope_p,
           lat_b, rope_b, qp, rs1, q_send, q_all, s_buf, p_buf, acc_send, o_buf,
           y_part, y_sib, y_send, y_all, piece, out_b,
           load_sem, own_sem, send_sem, recv_sem):
    ctx = lax.axis_index('ctx')
    core = lax.axis_index('seq')
    z, y, x = ctx // 16, (ctx // 4) % 4, ctx % 4
    colour = (x + y + z) % 4 + 4 * (y % 2)
    group = z * 2 + y // 2
    other = 1 - core
    row = 2 * colour + core
    dspan = hid_s.shape[2]
    cols = pl.ds(pl.multiple_of(colour * dspan, 128), dspan)
    heads = pl.ds(pl.multiple_of(group * 8, 8), 8)

    def dev(chip, c):
        return (0, chip, c)

    def remote(src, dst, phase, device):
        return pltpu.make_async_remote_copy(src_ref=src, dst_ref=dst, send_sem=send_sem.at[phase],
                                            recv_sem=recv_sem.at[phase], device_id=device,
                                            device_id_type=pl.DeviceIdType.MESH)

    def arrived(part, phase):
        remote(part, part, phase, dev(ctx, other)).wait_recv()

    def left(part, phase):
        remote(part, part, phase, dev(ctx, other)).wait_send()

    loads = [
        pltpu.make_async_copy(wuq.at[pl.ds(pl.multiple_of(colour * dspan, 128), dspan), heads, :], wq_s, load_sem.at[0]),
        pltpu.make_async_copy(wqr.at[heads, :, cols], wr_s, load_sem.at[1]),
        pltpu.make_async_copy(hidden.at[:, :, cols], hid_s, load_sem.at[2]),
        pltpu.make_async_copy(latent, lat_s, load_sem.at[3]),
        pltpu.make_async_copy(rope, rope_s, load_sem.at[4]),
        pltpu.make_async_copy(wuk.at[heads], wuk_s, load_sem.at[5]),
        pltpu.make_async_copy(wuv.at[heads], wuv_s, load_sem.at[6]),
        pltpu.make_async_copy(wout.at[heads], wout_s, load_sem.at[7]),
        pltpu.make_async_copy(lengths, len_s, load_sem.at[8]),
        pltpu.make_async_copy(hidden.at[row // 8], hid_r, load_sem.at[9]),
    ]
    for i in (0, 1, 2, 4, 3, 5):
        loads[i].start()

    barrier = pltpu.get_barrier_semaphore()

    def greet(chip, c):
        pl.semaphore_signal(barrier, inc=1, device_id=dev(chip, c), device_id_type=pl.DeviceIdType.MESH)

    me_class = core * 8 + group
    me_tile = colour * 2 + core
    for i in range(1, 16):
        peer = (me_class + i) % 16
        greet(chip_of(peer % 8, colour), peer // 8)
        peer = (me_tile + i) % 16
        greet(chip_of(group, peer // 2), peer % 2)
    sources = []
    for dx, dy, dz in SHIFTS:
        sources.append(chip_at((x + 4 - dx) % 4, (y + 4 - dy) % 4, (z + 4 - dz) % 4))
    for t in range(1, 8):
        for c in range(2):
            greet(sources[t], c)

    loads[0].wait()
    chunk = 64

    @pl.loop(0, dspan // chunk)
    def _(i):
        rows = wq_s[pl.ds(i * chunk, chunk)].astype(F32).reshape(chunk * 8, 128)
        wq_f[pl.ds(pl.multiple_of(i * chunk * 8, 8), chunk * 8), :] = rows

    loads[1].wait()
    loads[2].wait()
    hid = hid_s[...].astype(F32).reshape(16, dspan).astype(BF16)
    for h in range(8):
        w_h = wq_f[pl.ds(h, dspan, stride=8), :].astype(BF16)
        qp[0, pl.ds(h, 16, stride=8), :] = jnp.dot(hid, w_h, preferred_element_type=F32)
    part_r = lax.dot_general(hid, wr_s[...].reshape(512, dspan), NT, preferred_element_type=F32)
    for pair in range(4):
        both = part_r[:, pair * 128:(pair + 1) * 128]
        qp[1, pl.ds(2 * pair, 16, stride=8), :] = both
        qp[1, pl.ds(2 * pair + 1, 16, stride=8), :] = pltpu.roll(both, 64, 1)
    loads[4].wait()
    for b in range(16):
        rope_p[b] = jnp.concatenate([rope_s[b, 0:32, :], rope_s[b, 32:64, :]], axis=1)
    loads[3].wait()

    pl.semaphore_wait(barrier, 44)

    def pair_rows(c):
        return pl.ds(pl.multiple_of(c * 16, 16), 16)

    for i in range(1, 8):
        peer = (colour + i) % 8
        remote(qp.at[:, pair_rows(peer), :], rs1.at[colour], 0, dev(chip_of(group, peer), core)).start()

    def cache_send(t, c):
        dx, dy, dz = SHIFTS[t]
        chip = chip_at((x + 4 + dx) % 4, (y + 4 + dy) % 4, (z + 4 + dz) % 4)
        target = (colour + STEPS[t][0]) % 4 + 4 * ((colour // 4 + STEPS[t][1]) % 2)
        src_row = 2 * target + c
        slot = 2 * t + core
        remote(lat_s.at[src_row], lat_b.at[slot], 1, dev(chip, c)).start()
        remote(rope_p.at[src_row], rope_b.at[slot], 2, dev(chip, c)).start()

    for t in (5, 6, 7):
        for c in range(2):
            cache_send(t, c)
    cache_send(0, other)
    own_l = pltpu.make_async_copy(lat_s.at[row], lat_b.at[core], own_sem.at[0])
    own_r = pltpu.make_async_copy(rope_p.at[row], rope_b.at[core], own_sem.at[1])
    own_l.start()
    own_r.start()
    rs1[colour] = qp[:, pair_rows(colour), :]

    for i in (6, 7, 8, 9):
        loads[i].start()
    loads[5].wait()
    arrived(rs1.at[pl.ds(0, 7)], 0)
    total = rs1[0]
    for i in range(1, 8):
        total = total + rs1[i]
    q_nope = total[0].astype(BF16)
    q_rope = jnp.where(lax.broadcasted_iota(jnp.int32, (16, 128), 1) < 64, total[1], 0.0)
    row_head = lax.broadcasted_iota(jnp.int32, (16, 512), 0) % 8
    q_lat = jnp.zeros((16, 512), F32)
    for h in range(8):
        res = jnp.dot(q_nope, wuk_s[h], preferred_element_type=F32)
        q_lat = jnp.where(row_head == h, res, q_lat)
    for r in range(2):
        q_send[r, :, 0:512] = q_lat[r * 8:(r + 1) * 8].astype(BF16)
        q_send[r, :, 512:640] = q_rope[r * 8:(r + 1) * 8].astype(BF16)
    for i in range(1, 16):
        peer = (me_class + i) % 16
        remote(q_send.at[peer // 8], q_all.at[me_class], 3, dev(chip_of(peer % 8, colour), peer // 8)).start()
    for t in range(1, 5):
        for c in range(2):
            cache_send(t, c)
    q_all[me_class] = q_send[core]

    loads[8].wait()
    loads[9].wait()
    length = len_s[row]
    sub = lax.broadcasted_iota(jnp.int32, (8, dspan), 0)
    resid = jnp.zeros((8, dspan), F32)
    for i in range(8):
        block = hid_r[:, i * dspan:(i + 1) * dspan].astype(F32)
        line = jnp.sum(jnp.where(sub == row % 8, block, 0.0), axis=0, keepdims=True)
        resid = jnp.where(sub == i, line, resid)
    loads[6].wait()
    loads[7].wait()

    own_l.wait()
    own_r.wait()
    arrived(q_all.at[pl.ds(0, 15)], 3)
    arrived(lat_b.at[pl.ds(0, 15)], 1)
    arrived(rope_b.at[pl.ds(0, 15)], 2)
    queries = q_all[...].astype(F32).reshape(128, 640).astype(BF16)
    lane = lax.broadcasted_iota(jnp.int32, (128, 128), 1)
    top = None
    for t in range(8):
        keys = lat_b[2 * t:2 * t + 2].reshape(128, 512)
        packed = rope_b[2 * t:2 * t + 2]
        rkeys = jnp.concatenate([packed[:, :, 0:64], packed[:, :, 64:128]], axis=1).reshape(128, 64)
        s = lax.dot_general(queries[:, 0:512], keys, NT, preferred_element_type=F32)
        s = (s + lax.dot_general(queries[:, 512:576], rkeys, NT, preferred_element_type=F32)) * scale
        s = jnp.where(sources[t] * 128 + lane < length, s, NEG_FILL)
        s_buf[:, t * 128:(t + 1) * 128] = s
        m_t = jnp.max(s, axis=1, keepdims=True)
        top = m_t if top is None else jnp.maximum(top, m_t)
    den = jnp.zeros((128, 1), F32)
    for t in range(8):
        valid = sources[t] * 128 + lane < length
        w = jnp.where(valid, jnp.exp(s_buf[:, t * 128:(t + 1) * 128] - top), 0.0)
        den = den + jnp.sum(w, axis=1, keepdims=True)
        p_buf[:, t * 128:(t + 1) * 128] = w.astype(BF16)
    acc = jnp.dot(p_buf[...], lat_b[...].reshape(1024, 512), preferred_element_type=F32)
    acc_send[:, :, 0:512] = acc.reshape(16, 8, 512)
    acc_send[:, :, 512:640] = jnp.where(lane == 0, top, den).reshape(16, 8, 128)

    for i in range(1, 16):
        peer = (me_class + i) % 16
        remote(acc_send.at[peer], o_buf.at[me_class], 4, dev(chip_of(peer % 8, colour), peer // 8)).start()
    o_buf[me_class] = acc_send[me_class]
    arrived(o_buf.at[pl.ds(0, 15)], 4)
    finished = []
    for r in range(2):
        m_all = [o_buf[r * 8 + g, :, 512:513] for g in range(8)]
        best = functools.reduce(jnp.maximum, m_all)
        num = jnp.zeros((8, 512), F32)
        den_r = jnp.zeros((8, 1), F32)
        for g in range(8):
            factor = jnp.exp(m_all[g] - best)
            num = num + o_buf[r * 8 + g, :, 0:512] * factor
            den_r = den_r + o_buf[r * 8 + g, :, 513:514] * factor
        finished.append(num / den_r)
    o_lat = jnp.concatenate(finished, axis=0).astype(BF16)
    row_head = lax.broadcasted_iota(jnp.int32, (16, 128), 0) % 8
    vals = jnp.zeros((16, 128), F32)
    for h in range(8):
        res = jnp.dot(o_lat, wuv_s[h], preferred_element_type=F32)
        vals = jnp.where(row_head == h, res, vals)

    spread = jnp.concatenate([jnp.where(row_head == h, vals, 0.0) for h in range(8)], axis=1).astype(BF16)
    parts = [jnp.zeros((8, dspan), F32), jnp.zeros((8, dspan), F32)]
    for i in range(8):
        cut = wout_s[:, :, i * dspan:(i + 1) * dspan].reshape(1024, dspan)
        mixed = jnp.dot(spread, cut, preferred_element_type=F32)
        for r in range(2):
            line = jnp.sum(mixed[r * 8:(r + 1) * 8], axis=0, keepdims=True)
            parts[r] = jnp.where(sub == i, line, parts[r])
    y_part[0] = parts[0]
    y_part[1] = parts[1]
    remote(y_part.at[other], y_sib, 5, dev(ctx, other)).start()
    arrived(y_sib, 5)
    y_send[...] = y_part[core] + y_sib[...]
    for i in range(1, 8):
        peer = (group + i) % 8
        remote(y_send, y_all.at[group], 6, dev(chip_of(peer, colour), core)).start()
    y_all[group] = y_send[...]
    arrived(y_all.at[pl.ds(0, 7)], 6)
    y_sum = y_all[0]
    for g in range(1, 8):
        y_sum = y_sum + y_all[g]
    piece[...] = (resid + y_sum).astype(BF16)
    for i in range(1, 16):
        peer = (me_tile + i) % 16
        remote(piece, out_b.at[me_tile], 7, dev(chip_of(group, peer // 2), peer % 2)).start()
    out_b[me_tile] = piece[...]
    arrived(out_b.at[pl.ds(0, 15)], 7)
    out[...] = out_b[...]
    left(rs1.at[pl.ds(0, 7)], 0)
    left(lat_b.at[pl.ds(0, 15)], 1)
    left(rope_b.at[pl.ds(0, 15)], 2)
    left(q_all.at[pl.ds(0, 15)], 3)
    left(o_buf.at[pl.ds(0, 15)], 4)
    left(y_sib, 5)
    left(y_all.at[pl.ds(0, 7)], 6)
    left(out_b.at[pl.ds(0, 15)], 7)


def solution(mesh):
    row_spec = P('batch', None)
    cache_spec = P('batch', ('ctx', 'seq'), None)
    proj_spec = P(None, 'seq', None)
    head_spec = P('seq', None, None)

    def local_step(hidden, lengths, latent_cache, rope_keys, w_uq, w_qr, w_uk, w_uv, w_out):
        scale = (w_uq.shape[2] + w_qr.shape[2]) ** -0.5
        width = hidden.shape[1]
        dspan = width // 8
        vmem, dma = pltpu.VMEM, pltpu.SemaphoreType.DMA
        anywhere = pl.BlockSpec(memory_space=pl.ANY)
        scratch = [
            pltpu.SMEM((16,), jnp.int32),
            vmem((2, 8, dspan), BF16),
            vmem((8, width), BF16),
            vmem((dspan, 8, 128), BF16),
            vmem((dspan * 8, 128), F32),
            vmem((8, 64, dspan), BF16),
            vmem((8, 128, 512), BF16),
            vmem((8, 512, 128), BF16),
            vmem((8, 128, width), BF16),
            vmem((16, 64, 512), BF16),
            vmem((16, 64, 64), BF16),
            vmem((16, 32, 128), BF16),
            vmem((16, 64, 512), BF16),
            vmem((16, 32, 128), BF16),
            vmem((2, 128, 128), F32),
            vmem((8, 2, 16, 128), F32),
            vmem((2, 8, 640), BF16),
            vmem((16, 8, 640), BF16),
            vmem((128, 1024), F32),
            vmem((128, 1024), BF16),
            vmem((16, 8, 640), F32),
            vmem((16, 8, 640), F32),
            vmem((2, 8, dspan), F32),
            vmem((8, dspan), F32),
            vmem((8, dspan), F32),
            vmem((8, 8, dspan), F32),
            vmem((8, dspan), BF16),
            vmem((16, 8, dspan), BF16),
            dma((10,)), dma((2,)), dma((8,)), dma((8,)),
        ]
        out = pl.pallas_call(
            functools.partial(kernel, scale),
            out_shape=jax.ShapeDtypeStruct((16, 8, dspan), BF16),
            in_specs=[anywhere] * 9,
            out_specs=pl.BlockSpec(memory_space=pltpu.VMEM),
            scratch_shapes=scratch,
            compiler_params=pltpu.CompilerParams(collective_id=0, has_side_effects=True,
                                                 vmem_limit_bytes=67043328),
            name='mla_decode',
        )(hidden.reshape(2, 8, width), lengths, latent_cache, rope_keys, w_uq,
          jnp.transpose(w_qr, (1, 2, 0)), w_uk, w_uv, w_out)
        return out.reshape(16, width)

    return jax.shard_map(local_step, mesh=mesh,
                         in_specs=(row_spec, P('batch'), cache_spec, cache_spec, proj_spec, proj_spec, head_spec, head_spec, head_spec),
                         out_specs=row_spec, check_vma=False)
```

```python
import functools

import jax
import jax.numpy as jnp
from jax import lax
from jax.experimental import pallas as pl
from jax.experimental.pallas import tpu as pltpu
from jax.sharding import PartitionSpec as P

NEG_FILL = -1.0e30
F32 = jnp.float32
BF16 = jnp.bfloat16

SHIFTS = ((0, 0, 0), (1, 0, 0), (0, 0, -1), (0, 1, 0), (0, -1, 0), (-1, 0, -1), (1, -1, 0), (0, 1, 1))
STEPS = ((0, 0), (1, 0), (3, 0), (1, 1), (3, 1), (2, 0), (0, 1), (2, 1))

NT = (((1,), (1,)), ((), ()))


CLASS = ((2, 2, 0), (0, 2, 2), (2, 0, 2), (1, 2, 1), (3, 2, 3), (1, 0, 3), (3, 0, 1))


def kernel(scale, hidden, lengths, latent, rope, wuq, wqr, wuk, wuv, wout, out,
           len_s, hid_s, hid_r, wq_s, wq_f, wr_s, wuk_s, wuv_s, wout_s, lat_s, rope_s, rope_p,
           lat_b, rope_b, qp, rs1, q_send, q_all, s_buf, p_buf, acc_send, o_buf, ml_send, ml_all, ml_t,
           part_a, part_b, sib_a, sib_b, ysend_a, ysend_b, yall_a, yall_b, piece_a, piece_b, out_a, out_b,
           load_sem, own_sem, send_sem, recv_sem):
    ctx = lax.axis_index('ctx')
    core = lax.axis_index('seq')
    z, y, x = ctx // 16, (ctx // 4) % 4, ctx % 4
    xs = [(x + d) % 4 for d in range(4)]
    ys = [(y + d) % 4 for d in range(4)]
    zs = [(z + d) % 4 for d in range(4)]
    ys4 = [v * 4 for v in ys]
    zs16 = [v * 16 for v in zs]

    def chip_at(offset, sign=1):
        dx, dy, dz = offset
        return zs16[sign * dz % 4] + ys4[sign * dy % 4] + xs[sign * dx % 4]

    colour = (x + y + z) % 4 + 4 * (y % 2)
    group = z * 2 + y // 2
    other = 1 - core
    row = 2 * colour + core
    dspan = hid_s.shape[2]
    cols = pl.ds(pl.multiple_of(colour * dspan, 128), dspan)
    heads = pl.ds(pl.multiple_of(group * 8, 8), 8)

    def dev(chip, c):
        return (0, chip, c)

    def remote(src, dst, phase, device):
        return pltpu.make_async_remote_copy(src_ref=src, dst_ref=dst, send_sem=send_sem.at[phase],
                                            recv_sem=recv_sem.at[phase], device_id=device,
                                            device_id_type=pl.DeviceIdType.MESH)

    def arrived(part, phase):
        remote(part, part, phase, dev(ctx, other)).wait_recv()

    def left(part, phase):
        remote(part, part, phase, dev(ctx, other)).wait_send()

    loads = [
        pltpu.make_async_copy(wuq.at[pl.ds(pl.multiple_of(colour * dspan, 128), dspan), heads, :], wq_s, load_sem.at[0]),
        pltpu.make_async_copy(wqr.at[heads, :, cols], wr_s, load_sem.at[1]),
        pltpu.make_async_copy(hidden.at[:, :, cols], hid_s, load_sem.at[2]),
        pltpu.make_async_copy(latent, lat_s, load_sem.at[3]),
        pltpu.make_async_copy(rope, rope_s, load_sem.at[4]),
        pltpu.make_async_copy(wuk.at[heads], wuk_s, load_sem.at[5]),
        pltpu.make_async_copy(wuv.at[heads], wuv_s, load_sem.at[6]),
        pltpu.make_async_copy(wout.at[heads], wout_s, load_sem.at[7]),
        pltpu.make_async_copy(lengths, len_s, load_sem.at[8]),
        pltpu.make_async_copy(hidden.at[row // 8], hid_r, load_sem.at[9]),
    ]
    for i in (0, 1, 2, 4, 3, 5):
        loads[i].start()

    barrier = pltpu.get_barrier_semaphore()

    def greet(chip, c):
        pl.semaphore_signal(barrier, inc=1, device_id=dev(chip, c), device_id_type=pl.DeviceIdType.MESH)

    me_class = core * 8 + group
    me_tile = colour * 2 + core
    class_chips = [(chip_at(o), zs[o[2]] * 2 + ys[o[1]] // 2) for o in CLASS]
    class_peers = [(chip, c, c * 8 + g) for chip, g in class_chips for c in range(2)] + [(ctx, other, other * 8 + group)]
    mate = y + 1 - 2 * (y % 2)
    tile_chips = []
    for d in (2, 1, 3):
        tile_chips.append((z * 16 + mate * 4 + xs[d], (xs[d] + mate + z) % 4 + 4 * (mate % 2)))
    tile_chips.append((zs16[0] + ys4[0] + xs[2], (xs[2] + y + z) % 4 + 4 * (y % 2)))
    tile_chips.append((z * 16 + mate * 4 + x, (x + mate + z) % 4 + 4 * (mate % 2)))
    for d in (1, 3):
        tile_chips.append((zs16[0] + ys4[0] + xs[d], (xs[d] + y + z) % 4 + 4 * (y % 2)))
    tile_peers = [(chip, c, j) for chip, j in tile_chips for c in range(2)] + [(ctx, other, colour)]
    for chip, c, _ in class_peers[:-1]:
        greet(chip, c)
    for chip, c, _ in tile_peers:
        greet(chip, c)
    sources = [chip_at(o, -1) for o in SHIFTS]
    for t in (5, 6, 7, 1, 2, 3, 4):
        for c in range(2):
            greet(sources[t], c)

    loads[0].wait()
    chunk = 64

    @pl.loop(0, dspan // chunk)
    def _(i):
        rows = wq_s[pl.ds(i * chunk, chunk)].astype(F32).reshape(chunk * 8, 128)
        wq_f[pl.ds(pl.multiple_of(i * chunk * 8, 8), chunk * 8), :] = rows

    loads[1].wait()
    loads[2].wait()
    hid = hid_s[...].astype(F32).reshape(16, dspan).astype(BF16)
    for h in range(8):
        w_h = wq_f[pl.ds(h, dspan, stride=8), :].astype(BF16)
        qp[0, pl.ds(h, 16, stride=8), :] = jnp.dot(hid, w_h, preferred_element_type=F32)
    part_r = lax.dot_general(hid, wr_s[...].reshape(512, dspan), NT, preferred_element_type=F32)
    for pair in range(4):
        both = part_r[:, pair * 128:(pair + 1) * 128]
        qp[1, pl.ds(2 * pair, 16, stride=8), :] = both
        qp[1, pl.ds(2 * pair + 1, 16, stride=8), :] = pltpu.roll(both, 64, 1)
    loads[4].wait()
    for b in range(16):
        rope_p[b] = jnp.concatenate([rope_s[b, 0:32, :], rope_s[b, 32:64, :]], axis=1)
    loads[3].wait()

    pl.semaphore_wait(barrier, 43)

    def pair_rows(c):
        return pl.ds(pl.multiple_of(c * 16, 16), 16)

    for chip, peer in tile_chips:
        remote(qp.at[:, pair_rows(peer), :], rs1.at[colour], 0, dev(chip, core)).start()

    def cache_send(t, c):
        chip = chip_at(SHIFTS[t])
        target = (colour + STEPS[t][0]) % 4 + 4 * ((colour // 4 + STEPS[t][1]) % 2)
        src_row = 2 * target + c
        slot = 2 * t + core
        remote(lat_s.at[src_row], lat_b.at[slot], 1, dev(chip, c)).start()
        remote(rope_p.at[src_row], rope_b.at[slot], 2, dev(chip, c)).start()

    for t in (5, 6, 7):
        for c in range(2):
            cache_send(t, c)
    cache_send(0, other)
    own_l = pltpu.make_async_copy(lat_s.at[row], lat_b.at[core], own_sem.at[0])
    own_r = pltpu.make_async_copy(rope_p.at[row], rope_b.at[core], own_sem.at[1])
    own_l.start()
    own_r.start()
    rs1[colour] = qp[:, pair_rows(colour), :]

    for i in (6, 7, 8, 9):
        loads[i].start()
    loads[5].wait()
    arrived(rs1.at[pl.ds(0, 7)], 0)
    total = rs1[0]
    for i in range(1, 8):
        total = total + rs1[i]
    q_nope = total[0].astype(BF16)
    q_rope = jnp.where(lax.broadcasted_iota(jnp.int32, (16, 128), 1) < 64, total[1], 0.0)
    row_head = lax.broadcasted_iota(jnp.int32, (16, 512), 0) % 8
    q_lat = jnp.zeros((16, 512), F32)
    for h in range(8):
        res = jnp.dot(q_nope, wuk_s[h], preferred_element_type=F32)
        q_lat = jnp.where(row_head == h, res, q_lat)
    for r in range(2):
        q_send[r, :, 0:512] = q_lat[r * 8:(r + 1) * 8].astype(BF16)
        q_send[r, :, 512:640] = q_rope[r * 8:(r + 1) * 8].astype(BF16)
    for chip, c, _ in class_peers:
        remote(q_send.at[c], q_all.at[me_class], 3, dev(chip, c)).start()
    for t in range(1, 5):
        for c in range(2):
            cache_send(t, c)
    q_all[me_class] = q_send[core]

    loads[8].wait()
    loads[9].wait()
    length = len_s[row]
    sub = lax.broadcasted_iota(jnp.int32, (8, dspan), 0)
    resid = jnp.zeros((8, dspan), F32)
    for i in range(8):
        block = hid_r[:, i * dspan:(i + 1) * dspan].astype(F32)
        line = jnp.sum(jnp.where(sub == row % 8, block, 0.0), axis=0, keepdims=True)
        resid = jnp.where(sub == i, line, resid)
    loads[6].wait()
    loads[7].wait()

    own_l.wait()
    own_r.wait()
    arrived(q_all.at[pl.ds(0, 15)], 3)
    arrived(lat_b.at[pl.ds(0, 15)], 1)
    arrived(rope_b.at[pl.ds(0, 15)], 2)
    queries = q_all[...].astype(F32).reshape(128, 640).astype(BF16)
    lane = lax.broadcasted_iota(jnp.int32, (128, 128), 1)
    top = None
    for t in range(8):
        keys = lat_b[2 * t:2 * t + 2].reshape(128, 512)
        packed = rope_b[2 * t:2 * t + 2]
        rkeys = jnp.concatenate([packed[:, :, 0:64], packed[:, :, 64:128]], axis=1).reshape(128, 64)
        s = lax.dot_general(queries[:, 0:512], keys, NT, preferred_element_type=F32)
        s = (s + lax.dot_general(queries[:, 512:576], rkeys, NT, preferred_element_type=F32)) * scale
        s = jnp.where(sources[t] * 128 + lane < length, s, NEG_FILL)
        s_buf[:, t * 128:(t + 1) * 128] = s
        m_t = jnp.max(s, axis=1, keepdims=True)
        top = m_t if top is None else jnp.maximum(top, m_t)
    den = jnp.zeros((128, 1), F32)
    for t in range(8):
        valid = sources[t] * 128 + lane < length
        w = jnp.where(valid, jnp.exp(s_buf[:, t * 128:(t + 1) * 128] - top), 0.0)
        den = den + jnp.sum(w, axis=1, keepdims=True)
        p_buf[:, t * 128:(t + 1) * 128] = w.astype(BF16)
    acc = jnp.dot(p_buf[...], lat_b[...].reshape(1024, 512), preferred_element_type=F32)
    acc_send[...] = acc.reshape(16, 8, 512)
    ml_send[...] = jnp.where(lane == 0, top, den).T[0:2]

    for chip, c, _ in class_peers:
        remote(ml_send, ml_all.at[me_class], 5, dev(chip, c)).start()
    for chip, c, peer in class_peers:
        remote(acc_send.at[peer], o_buf.at[me_class], 4, dev(chip, c)).start()
    o_buf[me_class] = acc_send[me_class]
    ml_all[me_class] = ml_send[...]
    arrived(ml_all.at[pl.ds(0, 15)], 5)
    ml_t[:, 0:32] = ml_all[...].reshape(32, 128).T
    ml = ml_t[pl.ds(pl.multiple_of(me_class * 8, 8), 8), :]
    arrived(o_buf.at[pl.ds(0, 15)], 4)
    finished = []
    for r in range(2):
        m_all = [ml[:, 2 * (r * 8 + g):2 * (r * 8 + g) + 1] for g in range(8)]
        best = functools.reduce(jnp.maximum, m_all)
        num = jnp.zeros((8, 512), F32)
        den_r = jnp.zeros((8, 1), F32)
        for g in range(8):
            factor = jnp.exp(m_all[g] - best)
            num = num + o_buf[r * 8 + g] * factor
            den_r = den_r + ml[:, 2 * (r * 8 + g) + 1:2 * (r * 8 + g) + 2] * factor
        finished.append(num / den_r)
    o_lat = jnp.concatenate(finished, axis=0).astype(BF16)
    row_head = lax.broadcasted_iota(jnp.int32, (16, 128), 0) % 8
    vals = jnp.zeros((16, 128), F32)
    for h in range(8):
        res = jnp.dot(o_lat, wuv_s[h], preferred_element_type=F32)
        vals = jnp.where(row_head == h, res, vals)

    spread = jnp.concatenate([jnp.where(row_head == h, vals, 0.0) for h in range(8)], axis=1).astype(BF16)

    def y_chunk(part, start, phase, sib):
        size = part.shape[2]
        piece_of = lax.broadcasted_iota(jnp.int32, (8, size), 0)
        sums = [jnp.zeros((8, size), F32), jnp.zeros((8, size), F32)]
        for i in range(0, 8, 2):
            cut = jnp.concatenate([wout_s[:, :, k * dspan + start:k * dspan + start + size].reshape(1024, size)
                                   for k in (i, i + 1)], axis=1)
            mixed = jnp.dot(spread, cut, preferred_element_type=F32)
            for k in range(2):
                for r in range(2):
                    line = jnp.sum(mixed[r * 8:(r + 1) * 8, k * size:(k + 1) * size], axis=0, keepdims=True)
                    sums[r] = jnp.where(piece_of == i + k, line, sums[r])
        part[0] = sums[0]
        part[1] = sums[1]
        remote(part.at[other], sib, phase, dev(ctx, other)).start()

    def y_share(part, sib, ysend, yall, swap_phase, phase):
        arrived(sib, swap_phase)
        ysend[...] = part[core] + sib[...]
        for chip, _ in class_chips:
            remote(ysend, yall.at[group], phase, dev(chip, core)).start()
        yall[group] = ysend[...]

    def out_share(yall, piece, dest, start, y_phase, phase):
        arrived(yall.at[pl.ds(0, 7)], y_phase)
        y_sum = yall[0]
        for g in range(1, 8):
            y_sum = y_sum + yall[g]
        piece[...] = (resid[:, start:start + piece.shape[1]] + y_sum).astype(BF16)
        for chip, c, _ in tile_peers:
            remote(piece, dest.at[me_tile], phase, dev(chip, c)).start()
        dest[me_tile] = piece[...]

    first = part_a.shape[2]
    y_chunk(part_a, 0, 6, sib_a)
    y_chunk(part_b, first, 7, sib_b)
    y_share(part_a, sib_a, ysend_a, yall_a, 6, 8)
    y_share(part_b, sib_b, ysend_b, yall_b, 7, 9)
    out_share(yall_a, piece_a, out_a, 0, 8, 10)
    out_share(yall_b, piece_b, out_b, first, 9, 11)
    arrived(out_a.at[pl.ds(0, 15)], 10)
    out[:, :, 0:first] = out_a[...]
    arrived(out_b.at[pl.ds(0, 15)], 11)
    out[:, :, first:dspan] = out_b[...]
    left(rs1.at[pl.ds(0, 7)], 0)
    left(lat_b.at[pl.ds(0, 15)], 1)
    left(rope_b.at[pl.ds(0, 15)], 2)
    left(q_all.at[pl.ds(0, 15)], 3)
    left(o_buf.at[pl.ds(0, 15)], 4)
    left(ml_all.at[pl.ds(0, 15)], 5)
    left(sib_a, 6)
    left(sib_b, 7)
    left(yall_a.at[pl.ds(0, 7)], 8)
    left(yall_b.at[pl.ds(0, 7)], 9)
    left(out_a.at[pl.ds(0, 15)], 10)
    left(out_b.at[pl.ds(0, 15)], 11)


def solution(mesh):
    row_spec = P('batch', None)
    cache_spec = P('batch', ('ctx', 'seq'), None)
    proj_spec = P(None, 'seq', None)
    head_spec = P('seq', None, None)

    def local_step(hidden, lengths, latent_cache, rope_keys, w_uq, w_qr, w_uk, w_uv, w_out):
        scale = (w_uq.shape[2] + w_qr.shape[2]) ** -0.5
        width = hidden.shape[1]
        dspan = width // 8
        first = dspan // 128 // 2 * 128 + 128
        second = dspan - first
        vmem, dma = pltpu.VMEM, pltpu.SemaphoreType.DMA
        anywhere = pl.BlockSpec(memory_space=pl.ANY)
        scratch = [
            pltpu.SMEM((16,), jnp.int32),
            vmem((2, 8, dspan), BF16),
            vmem((8, width), BF16),
            vmem((dspan, 8, 128), BF16),
            vmem((dspan * 8, 128), F32),
            vmem((8, 64, dspan), BF16),
            vmem((8, 128, 512), BF16),
            vmem((8, 512, 128), BF16),
            vmem((8, 128, width), BF16),
            vmem((16, 64, 512), BF16),
            vmem((16, 64, 64), BF16),
            vmem((16, 32, 128), BF16),
            vmem((16, 64, 512), BF16),
            vmem((16, 32, 128), BF16),
            vmem((2, 128, 128), F32),
            vmem((8, 2, 16, 128), F32),
            vmem((2, 8, 640), BF16),
            vmem((16, 8, 640), BF16),
            vmem((128, 1024), F32),
            vmem((128, 1024), BF16),
            vmem((16, 8, 512), F32),
            vmem((16, 8, 512), F32),
            vmem((2, 128), F32),
            vmem((16, 2, 128), F32),
            vmem((128, 128), F32),
            vmem((2, 8, first), F32),
            vmem((2, 8, second), F32),
            vmem((8, first), F32),
            vmem((8, second), F32),
            vmem((8, first), F32),
            vmem((8, second), F32),
            vmem((8, 8, first), F32),
            vmem((8, 8, second), F32),
            vmem((8, first), BF16),
            vmem((8, second), BF16),
            vmem((16, 8, first), BF16),
            vmem((16, 8, second), BF16),
            dma((10,)), dma((2,)), dma((12,)), dma((12,)),
        ]
        out = pl.pallas_call(
            functools.partial(kernel, scale),
            out_shape=jax.ShapeDtypeStruct((16, 8, dspan), BF16),
            in_specs=[anywhere] * 9,
            out_specs=pl.BlockSpec(memory_space=pltpu.VMEM),
            scratch_shapes=scratch,
            compiler_params=pltpu.CompilerParams(collective_id=0, has_side_effects=True,
                                                 vmem_limit_bytes=67043328),
            name='mla_decode',
        )(hidden.reshape(2, 8, width), lengths, latent_cache, rope_keys, w_uq,
          jnp.transpose(w_qr, (1, 2, 0)), w_uk, w_uv, w_out)
        return out.reshape(16, width)

    return jax.shard_map(local_step, mesh=mesh,
                         in_specs=(row_spec, P('batch'), cache_spec, cache_spec, proj_spec, proj_spec, head_spec, head_spec, head_spec),
                         out_specs=row_spec, check_vma=False)
```

```python
import functools

import jax
import jax.numpy as jnp
from jax import lax
from jax.experimental import pallas as pl
from jax.experimental.pallas import tpu as pltpu
from jax.sharding import PartitionSpec as P

NEG_FILL = -1.0e30
F32 = jnp.float32
BF16 = jnp.bfloat16

SHIFTS = ((0, 0, 0), (1, 0, 0), (0, 0, -1), (0, 1, 0), (0, -1, 0), (-1, 0, -1), (1, -1, 0), (0, 1, 1))
STEPS = ((0, 0), (1, 0), (3, 0), (1, 1), (3, 1), (2, 0), (0, 1), (2, 1))

NT = (((1,), (1,)), ((), ()))


CLASS = ((2, 2, 0), (0, 2, 2), (2, 0, 2), (1, 2, 1), (3, 2, 3), (1, 0, 3), (3, 0, 1))
NEAR = ((0, 1, 0), (0, 3, 0), (0, 0, 1), (0, 0, 3), (1, 0, 1), (3, 0, 3), (1, 3, 0), (3, 1, 0), (0, 1, 1), (0, 3, 3),
        (1, 1, 0), (3, 3, 0))
RELAY = ((0, 1, 1), (0, 3, 3), (1, 0, 1), (1, 3, 0), (1, 0, 0), (3, 0, 0))


def kernel(scale, hidden, lengths, latent, rope, wuq, wqr, wuk, wuv, wout, out,
           len_s, hid_s, hid_r, wq_s, wq_f, wr_s, wuk_s, wuv_s, wout_s, lat_s, rope_s, rope_p,
           lat_b, rope_b, qp, rs1, q_send, q_all, s_buf, p_buf, acc_send, o_buf, ml_send, ml_all, ml_t,
           part_a, part_b, sib_a, sib_b, ysend_a, ysend_b, yall_a, yall_b, piece_a, piece_b, out_a, out_b,
           load_sem, own_sem, send_sem, recv_sem, near_sem):
    ctx = lax.axis_index('ctx')
    core = lax.axis_index('seq')
    z, y, x = ctx // 16, (ctx // 4) % 4, ctx % 4
    xs = [(x + d) % 4 for d in range(4)]
    ys = [(y + d) % 4 for d in range(4)]
    zs = [(z + d) % 4 for d in range(4)]
    ys4 = [v * 4 for v in ys]
    zs16 = [v * 16 for v in zs]

    def chip_at(offset, sign=1):
        dx, dy, dz = offset
        return zs16[sign * dz % 4] + ys4[sign * dy % 4] + xs[sign * dx % 4]

    colour = (x + y + z) % 4 + 4 * (y % 2)
    group = z * 2 + y // 2
    other = 1 - core
    row = 2 * colour + core
    dspan = hid_s.shape[2]
    cols = pl.ds(pl.multiple_of(colour * dspan, 128), dspan)
    heads = pl.ds(pl.multiple_of(group * 8, 8), 8)

    def dev(chip, c):
        return (0, chip, c)

    def remote(src, dst, phase, device):
        return pltpu.make_async_remote_copy(src_ref=src, dst_ref=dst, send_sem=send_sem.at[phase],
                                            recv_sem=recv_sem.at[phase], device_id=device,
                                            device_id_type=pl.DeviceIdType.MESH)

    def arrived(part, phase):
        remote(part, part, phase, dev(ctx, other)).wait_recv()

    def left(part, phase):
        remote(part, part, phase, dev(ctx, other)).wait_send()

    loads = [
        pltpu.make_async_copy(wuq.at[pl.ds(pl.multiple_of(colour * dspan, 128), dspan), heads, :], wq_s, load_sem.at[0]),
        pltpu.make_async_copy(wqr.at[heads, :, cols], wr_s, load_sem.at[1]),
        pltpu.make_async_copy(hidden.at[:, :, cols], hid_s, load_sem.at[2]),
        pltpu.make_async_copy(latent, lat_s, load_sem.at[3]),
        pltpu.make_async_copy(rope, rope_s, load_sem.at[4]),
        pltpu.make_async_copy(wuk.at[heads], wuk_s, load_sem.at[5]),
        pltpu.make_async_copy(wuv.at[heads], wuv_s, load_sem.at[6]),
        pltpu.make_async_copy(wout.at[heads], wout_s, load_sem.at[7]),
        pltpu.make_async_copy(lengths, len_s, load_sem.at[8]),
        pltpu.make_async_copy(hidden.at[row // 8], hid_r, load_sem.at[9]),
    ]
    for i in (0, 1, 2, 4, 3, 5):
        loads[i].start()

    barrier = pltpu.get_barrier_semaphore()

    def greet(chip, c):
        pl.semaphore_signal(barrier, inc=1, device_id=dev(chip, c), device_id_type=pl.DeviceIdType.MESH)

    me_class = core * 8 + group
    me_tile = colour * 2 + core
    class_chips = [(chip_at(o), zs[o[2]] * 2 + ys[o[1]] // 2) for o in CLASS]
    class_peers = [(chip, c, c * 8 + g) for chip, g in class_chips for c in range(2)] + [(ctx, other, other * 8 + group)]
    mate = y + 1 - 2 * (y % 2)
    tile_chips = []
    for d in (2, 1, 3):
        tile_chips.append((z * 16 + mate * 4 + xs[d], (xs[d] + mate + z) % 4 + 4 * (mate % 2)))
    tile_chips.append((zs16[0] + ys4[0] + xs[2], (xs[2] + y + z) % 4 + 4 * (y % 2)))
    tile_chips.append((z * 16 + mate * 4 + x, (x + mate + z) % 4 + 4 * (mate % 2)))
    for d in (1, 3):
        tile_chips.append((zs16[0] + ys4[0] + xs[d], (xs[d] + y + z) % 4 + 4 * (y % 2)))
    tile_peers = [(chip, c, j) for chip, j in tile_chips for c in range(2)] + [(ctx, other, colour)]
    sources = [chip_at(o, -1) for o in SHIFTS]
    for chip, c, _ in tile_peers:
        greet(chip, c)
    for offset in NEAR:
        for c in range(2):
            greet(chip_at(offset), c)

    loads[0].wait()
    chunk = 64

    @pl.loop(0, dspan // chunk)
    def _(i):
        rows = wq_s[pl.ds(i * chunk, chunk)].astype(F32).reshape(chunk * 8, 128)
        wq_f[pl.ds(pl.multiple_of(i * chunk * 8, 8), chunk * 8), :] = rows

    loads[1].wait()
    loads[2].wait()
    hid = hid_s[...].astype(F32).reshape(16, dspan).astype(BF16)
    for h in range(8):
        w_h = wq_f[pl.ds(h, dspan, stride=8), :].astype(BF16)
        qp[0, pl.ds(h, 16, stride=8), :] = jnp.dot(hid, w_h, preferred_element_type=F32)
    part_r = lax.dot_general(hid, wr_s[...].reshape(512, dspan), NT, preferred_element_type=F32)
    for pair in range(4):
        both = part_r[:, pair * 128:(pair + 1) * 128]
        qp[1, pl.ds(2 * pair, 16, stride=8), :] = both
        qp[1, pl.ds(2 * pair + 1, 16, stride=8), :] = pltpu.roll(both, 64, 1)
    loads[4].wait()
    for b in range(16):
        rope_p[b] = jnp.concatenate([rope_s[b, 0:32, :], rope_s[b, 32:64, :]], axis=1)
    loads[3].wait()

    pl.semaphore_wait(barrier, 39)
    for offset in RELAY:
        pl.semaphore_signal(near_sem, inc=1, device_id=dev(chip_at(offset), core), device_id_type=pl.DeviceIdType.MESH)

    def pair_rows(c):
        return pl.ds(pl.multiple_of(c * 16, 16), 16)

    for chip, peer in tile_chips:
        remote(qp.at[:, pair_rows(peer), :], rs1.at[colour], 0, dev(chip, core)).start()

    def cache_send(t, c, late):
        chip = chip_at(SHIFTS[t])
        target = (colour + STEPS[t][0]) % 4 + 4 * ((colour // 4 + STEPS[t][1]) % 2)
        src_row = 2 * target + c
        slot = 2 * t + core
        remote(lat_s.at[src_row], lat_b.at[slot], 12 if late else 1, dev(chip, c)).start()
        remote(rope_p.at[src_row], rope_b.at[slot], 13 if late else 2, dev(chip, c)).start()

    for t in (5, 6, 7):
        for c in range(2):
            cache_send(t, c, False)
    cache_send(0, other, False)
    own_l = pltpu.make_async_copy(lat_s.at[row], lat_b.at[core], own_sem.at[0])
    own_r = pltpu.make_async_copy(rope_p.at[row], rope_b.at[core], own_sem.at[1])
    own_l.start()
    own_r.start()
    rs1[colour] = qp[:, pair_rows(colour), :]

    for i in (6, 7, 8, 9):
        loads[i].start()
    loads[5].wait()
    arrived(rs1.at[pl.ds(0, 7)], 0)
    total = rs1[0]
    for i in range(1, 8):
        total = total + rs1[i]
    q_nope = total[0].astype(BF16)
    q_rope = jnp.where(lax.broadcasted_iota(jnp.int32, (16, 128), 1) < 64, total[1], 0.0)
    row_head = lax.broadcasted_iota(jnp.int32, (16, 512), 0) % 8
    q_lat = jnp.zeros((16, 512), F32)
    for h in range(8):
        res = jnp.dot(q_nope, wuk_s[h], preferred_element_type=F32)
        q_lat = jnp.where(row_head == h, res, q_lat)
    for r in range(2):
        q_send[r, :, 0:512] = q_lat[r * 8:(r + 1) * 8].astype(BF16)
        q_send[r, :, 512:640] = q_rope[r * 8:(r + 1) * 8].astype(BF16)
    pl.semaphore_wait(near_sem, 6)
    for chip, c, _ in class_peers:
        remote(q_send.at[c], q_all.at[me_class], 3, dev(chip, c)).start()
    for t in range(1, 5):
        for c in range(2):
            cache_send(t, c, True)
    q_all[me_class] = q_send[core]

    loads[8].wait()
    loads[9].wait()
    length = len_s[row]
    sub = lax.broadcasted_iota(jnp.int32, (8, dspan), 0)
    resid = jnp.zeros((8, dspan), F32)
    for i in range(8):
        block = hid_r[:, i * dspan:(i + 1) * dspan].astype(F32)
        line = jnp.sum(jnp.where(sub == row % 8, block, 0.0), axis=0, keepdims=True)
        resid = jnp.where(sub == i, line, resid)
    loads[6].wait()
    loads[7].wait()

    own_l.wait()
    own_r.wait()
    arrived(q_all.at[pl.ds(0, 15)], 3)
    arrived(lat_b.at[pl.ds(0, 7)], 1)
    arrived(rope_b.at[pl.ds(0, 7)], 2)
    queries = q_all[...].astype(F32).reshape(128, 640).astype(BF16)
    lane = lax.broadcasted_iota(jnp.int32, (128, 128), 1)

    def scores(t):
        keys = lat_b[2 * t:2 * t + 2].reshape(128, 512)
        packed = rope_b[2 * t:2 * t + 2]
        rkeys = jnp.concatenate([packed[:, :, 0:64], packed[:, :, 64:128]], axis=1).reshape(128, 64)
        s = lax.dot_general(queries[:, 0:512], keys, NT, preferred_element_type=F32)
        s = (s + lax.dot_general(queries[:, 512:576], rkeys, NT, preferred_element_type=F32)) * scale
        s = jnp.where(sources[t] * 128 + lane < length, s, NEG_FILL)
        s_buf[:, t * 128:(t + 1) * 128] = s
        return jnp.max(s, axis=1, keepdims=True)

    top = functools.reduce(jnp.maximum, [scores(t) for t in (0, 5, 6, 7)])
    arrived(lat_b.at[pl.ds(0, 8)], 12)
    arrived(rope_b.at[pl.ds(0, 8)], 13)
    top = functools.reduce(jnp.maximum, [top] + [scores(t) for t in range(1, 5)])
    den = jnp.zeros((128, 1), F32)
    for t in range(8):
        valid = sources[t] * 128 + lane < length
        w = jnp.where(valid, jnp.exp(s_buf[:, t * 128:(t + 1) * 128] - top), 0.0)
        den = den + jnp.sum(w, axis=1, keepdims=True)
        p_buf[:, t * 128:(t + 1) * 128] = w.astype(BF16)
    ml_send[...] = jnp.where(lane == 0, top, den).T[0:2]
    acc = jnp.dot(p_buf[...], lat_b[...].reshape(1024, 512), preferred_element_type=F32)
    acc_send[...] = acc.reshape(16, 8, 512)

    for chip, c, _ in class_peers:
        remote(ml_send, ml_all.at[me_class], 5, dev(chip, c)).start()
    for chip, c, peer in class_peers:
        remote(acc_send.at[peer], o_buf.at[me_class], 4, dev(chip, c)).start()
    o_buf[me_class] = acc_send[me_class]
    ml_all[me_class] = ml_send[...]
    arrived(ml_all.at[pl.ds(0, 15)], 5)
    ml_t[:, 0:32] = ml_all[...].reshape(32, 128).T
    ml = ml_t[pl.ds(pl.multiple_of(me_class * 8, 8), 8), :]
    factors, dens = [], []
    for r in range(2):
        m_all = [ml[:, 2 * (r * 8 + g):2 * (r * 8 + g) + 1] for g in range(8)]
        best = functools.reduce(jnp.maximum, m_all)
        den_r = jnp.zeros((8, 1), F32)
        for g in range(8):
            factor = jnp.exp(m_all[g] - best)
            den_r = den_r + ml[:, 2 * (r * 8 + g) + 1:2 * (r * 8 + g) + 2] * factor
            factors.append(jnp.broadcast_to(factor, (8, 512)))
        dens.append(den_r)
    arrived(o_buf.at[pl.ds(0, 15)], 4)
    finished = []
    for r in range(2):
        num = jnp.zeros((8, 512), F32)
        for g in range(8):
            num = num + o_buf[r * 8 + g] * factors[r * 8 + g]
        finished.append(num / dens[r])
    o_lat = jnp.concatenate(finished, axis=0).astype(BF16)
    row_head = lax.broadcasted_iota(jnp.int32, (16, 128), 0) % 8
    vals = jnp.zeros((16, 128), F32)
    for h in range(8):
        res = jnp.dot(o_lat, wuv_s[h], preferred_element_type=F32)
        vals = jnp.where(row_head == h, res, vals)

    spread = jnp.concatenate([jnp.where(row_head == h, vals, 0.0) for h in range(8)], axis=1).astype(BF16)

    def y_chunk(part, start, phase, sib):
        size = part.shape[2]
        piece_of = lax.broadcasted_iota(jnp.int32, (8, size), 0)
        sums = [jnp.zeros((8, size), F32), jnp.zeros((8, size), F32)]
        for i in range(0, 8, 2):
            cut = jnp.concatenate([wout_s[:, :, k * dspan + start:k * dspan + start + size].reshape(1024, size)
                                   for k in (i, i + 1)], axis=1)
            mixed = jnp.dot(spread, cut, preferred_element_type=F32)
            for k in range(2):
                for r in range(2):
                    line = jnp.sum(mixed[r * 8:(r + 1) * 8, k * size:(k + 1) * size], axis=0, keepdims=True)
                    sums[r] = jnp.where(piece_of == i + k, line, sums[r])
        part[0] = sums[0]
        part[1] = sums[1]
        remote(part.at[other], sib, phase, dev(ctx, other)).start()

    def y_share(part, sib, ysend, yall, swap_phase, phase):
        arrived(sib, swap_phase)
        ysend[...] = part[core] + sib[...]
        for chip, _ in class_chips:
            remote(ysend, yall.at[group], phase, dev(chip, core)).start()
        yall[group] = ysend[...]

    def out_share(yall, piece, dest, start, y_phase, phase):
        arrived(yall.at[pl.ds(0, 7)], y_phase)
        y_sum = yall[0]
        for g in range(1, 8):
            y_sum = y_sum + yall[g]
        piece[...] = (resid[:, start:start + piece.shape[1]] + y_sum).astype(BF16)
        for chip, c, _ in tile_peers:
            remote(piece, dest.at[me_tile], phase, dev(chip, c)).start()
        dest[me_tile] = piece[...]

    first = part_a.shape[2]
    y_chunk(part_a, 0, 6, sib_a)
    y_chunk(part_b, first, 7, sib_b)
    y_share(part_a, sib_a, ysend_a, yall_a, 6, 8)
    y_share(part_b, sib_b, ysend_b, yall_b, 7, 9)
    out_share(yall_a, piece_a, out_a, 0, 8, 10)
    out_share(yall_b, piece_b, out_b, first, 9, 11)
    arrived(out_a.at[pl.ds(0, 15)], 10)
    out[:, :, 0:first] = out_a[...]
    arrived(out_b.at[pl.ds(0, 15)], 11)
    out[:, :, first:dspan] = out_b[...]
    left(rs1.at[pl.ds(0, 7)], 0)
    left(lat_b.at[pl.ds(0, 7)], 1)
    left(rope_b.at[pl.ds(0, 7)], 2)
    left(lat_b.at[pl.ds(0, 8)], 12)
    left(rope_b.at[pl.ds(0, 8)], 13)
    left(q_all.at[pl.ds(0, 15)], 3)
    left(o_buf.at[pl.ds(0, 15)], 4)
    left(ml_all.at[pl.ds(0, 15)], 5)
    left(sib_a, 6)
    left(sib_b, 7)
    left(yall_a.at[pl.ds(0, 7)], 8)
    left(yall_b.at[pl.ds(0, 7)], 9)
    left(out_a.at[pl.ds(0, 15)], 10)
    left(out_b.at[pl.ds(0, 15)], 11)


def solution(mesh):
    row_spec = P('batch', None)
    cache_spec = P('batch', ('ctx', 'seq'), None)
    proj_spec = P(None, 'seq', None)
    head_spec = P('seq', None, None)

    def local_step(hidden, lengths, latent_cache, rope_keys, w_uq, w_qr, w_uk, w_uv, w_out):
        scale = (w_uq.shape[2] + w_qr.shape[2]) ** -0.5
        width = hidden.shape[1]
        dspan = width // 8
        first = dspan // 128 // 2 * 128 + 128
        second = dspan - first
        vmem, dma = pltpu.VMEM, pltpu.SemaphoreType.DMA
        anywhere = pl.BlockSpec(memory_space=pl.ANY)
        scratch = [
            pltpu.SMEM((16,), jnp.int32),
            vmem((2, 8, dspan), BF16),
            vmem((8, width), BF16),
            vmem((dspan, 8, 128), BF16),
            vmem((dspan * 8, 128), F32),
            vmem((8, 64, dspan), BF16),
            vmem((8, 128, 512), BF16),
            vmem((8, 512, 128), BF16),
            vmem((8, 128, width), BF16),
            vmem((16, 64, 512), BF16),
            vmem((16, 64, 64), BF16),
            vmem((16, 32, 128), BF16),
            vmem((16, 64, 512), BF16),
            vmem((16, 32, 128), BF16),
            vmem((2, 128, 128), F32),
            vmem((8, 2, 16, 128), F32),
            vmem((2, 8, 640), BF16),
            vmem((16, 8, 640), BF16),
            vmem((128, 1024), F32),
            vmem((128, 1024), BF16),
            vmem((16, 8, 512), F32),
            vmem((16, 8, 512), F32),
            vmem((2, 128), F32),
            vmem((16, 2, 128), F32),
            vmem((128, 128), F32),
            vmem((2, 8, first), F32),
            vmem((2, 8, second), F32),
            vmem((8, first), F32),
            vmem((8, second), F32),
            vmem((8, first), F32),
            vmem((8, second), F32),
            vmem((8, 8, first), F32),
            vmem((8, 8, second), F32),
            vmem((8, first), BF16),
            vmem((8, second), BF16),
            vmem((16, 8, first), BF16),
            vmem((16, 8, second), BF16),
            dma((10,)), dma((2,)), dma((14,)), dma((14,)), pltpu.SemaphoreType.REGULAR,
        ]
        out = pl.pallas_call(
            functools.partial(kernel, scale),
            out_shape=jax.ShapeDtypeStruct((16, 8, dspan), BF16),
            in_specs=[anywhere] * 9,
            out_specs=pl.BlockSpec(memory_space=pltpu.VMEM),
            scratch_shapes=scratch,
            compiler_params=pltpu.CompilerParams(collective_id=0, has_side_effects=True,
                                                 vmem_limit_bytes=67043328),
            name='mla_decode',
        )(hidden.reshape(2, 8, width), lengths, latent_cache, rope_keys, w_uq,
          jnp.transpose(w_qr, (1, 2, 0)), w_uk, w_uv, w_out)
        return out.reshape(16, width)

    return jax.shard_map(local_step, mesh=mesh,
                         in_specs=(row_spec, P('batch'), cache_spec, cache_spec, proj_spec, proj_spec, head_spec, head_spec, head_spec),
                         out_specs=row_spec, check_vma=False)
```

```python
import functools

import jax
import jax.numpy as jnp
from jax import lax
from jax.experimental import pallas as pl
from jax.experimental.pallas import tpu as pltpu
from jax.sharding import PartitionSpec as P

NEG_FILL = -1.0e30
F32 = jnp.float32
BF16 = jnp.bfloat16

SHIFTS = ((0, 0, 0), (1, 0, 0), (0, 0, -1), (0, 1, 0), (0, -1, 0), (-1, 0, -1), (1, -1, 0), (0, 1, 1))
STEPS = ((0, 0), (1, 0), (3, 0), (1, 1), (3, 1), (2, 0), (0, 1), (2, 1))

NT = (((1,), (1,)), ((), ()))


CLASS = ((2, 2, 0), (0, 2, 2), (2, 0, 2), (1, 2, 1), (3, 2, 3), (1, 0, 3), (3, 0, 1))
NEAR = ((0, 1, 0), (0, 3, 0), (0, 0, 1), (0, 0, 3), (1, 0, 1), (3, 0, 3), (1, 3, 0), (3, 1, 0), (0, 1, 1), (0, 3, 3),
        (1, 1, 0), (3, 3, 0))
RELAY = ((0, 1, 1), (0, 3, 3), (1, 0, 1), (1, 3, 0), (1, 0, 0), (3, 0, 0))


def kernel(scale, hidden, lengths, latent, rope, wuq, wqr, wuk, wuv, wout, out,
           len_s, hid_s, hid_r, wq_s, wq_f, wr_s, wuk_s, wuv_s, wout_s, lat_s, rope_s, rope_p,
           lat_b, rope_b, qp, rs1, q_send, q_all, s_buf, p_buf, acc_send, o_buf, ml_send, ml_all, ml_t,
           part_a, part_b, sib_a, sib_b, ysend_a, ysend_b, yall_a, yall_b, piece_a, piece_b, out_a, out_b, rows_f,
           load_sem, own_sem, send_sem, recv_sem, near_sem):
    ctx = lax.axis_index('ctx')
    core = lax.axis_index('seq')
    z, y, x = ctx // 16, (ctx // 4) % 4, ctx % 4
    xs = [(x + d) % 4 for d in range(4)]
    ys = [(y + d) % 4 for d in range(4)]
    zs = [(z + d) % 4 for d in range(4)]
    ys4 = [v * 4 for v in ys]
    zs16 = [v * 16 for v in zs]

    def chip_at(offset, sign=1):
        dx, dy, dz = offset
        return zs16[sign * dz % 4] + ys4[sign * dy % 4] + xs[sign * dx % 4]

    colour = (x + y + z) % 4 + 4 * (y % 2)
    group = z * 2 + y // 2
    other = 1 - core
    row = 2 * colour + core
    dspan = hid_s.shape[2]
    cols = pl.ds(pl.multiple_of(colour * dspan, 128), dspan)
    heads = pl.ds(pl.multiple_of(group * 8, 8), 8)

    def dev(chip, c):
        return (0, chip, c)

    def remote(src, dst, phase, device):
        return pltpu.make_async_remote_copy(src_ref=src, dst_ref=dst, send_sem=send_sem.at[phase],
                                            recv_sem=recv_sem.at[phase], device_id=device,
                                            device_id_type=pl.DeviceIdType.MESH)

    def arrived(part, phase):
        remote(part, part, phase, dev(ctx, other)).wait_recv()

    def left(part, phase):
        remote(part, part, phase, dev(ctx, other)).wait_send()

    loads = [
        pltpu.make_async_copy(wuq.at[pl.ds(pl.multiple_of(colour * dspan, 128), dspan), heads, :], wq_s, load_sem.at[0]),
        pltpu.make_async_copy(wqr.at[heads, :, cols], wr_s, load_sem.at[1]),
        pltpu.make_async_copy(hidden.at[:, :, cols], hid_s, load_sem.at[2]),
        pltpu.make_async_copy(latent, lat_s, load_sem.at[3]),
        pltpu.make_async_copy(rope, rope_s, load_sem.at[4]),
        pltpu.make_async_copy(wuk.at[heads], wuk_s, load_sem.at[5]),
        pltpu.make_async_copy(wuv.at[heads], wuv_s, load_sem.at[6]),
        pltpu.make_async_copy(wout.at[heads], wout_s, load_sem.at[7]),
        pltpu.make_async_copy(lengths, len_s, load_sem.at[8]),
        pltpu.make_async_copy(hidden.at[row // 8], hid_r, load_sem.at[9]),
    ]
    for i in (0, 1, 2, 4, 3, 5):
        loads[i].start()

    barrier = pltpu.get_barrier_semaphore()

    def greet(chip, c):
        pl.semaphore_signal(barrier, inc=1, device_id=dev(chip, c), device_id_type=pl.DeviceIdType.MESH)

    me_class = core * 8 + group
    me_tile = colour * 2 + core
    class_chips = [(chip_at(o), zs[o[2]] * 2 + ys[o[1]] // 2) for o in CLASS]
    class_peers = [(chip, c, c * 8 + g) for chip, g in class_chips for c in range(2)] + [(ctx, other, other * 8 + group)]
    mate = y + 1 - 2 * (y % 2)
    tile_chips = []
    for d in (2, 1, 3):
        tile_chips.append((z * 16 + mate * 4 + xs[d], (xs[d] + mate + z) % 4 + 4 * (mate % 2)))
    tile_chips.append((zs16[0] + ys4[0] + xs[2], (xs[2] + y + z) % 4 + 4 * (y % 2)))
    tile_chips.append((z * 16 + mate * 4 + x, (x + mate + z) % 4 + 4 * (mate % 2)))
    for d in (1, 3):
        tile_chips.append((zs16[0] + ys4[0] + xs[d], (xs[d] + y + z) % 4 + 4 * (y % 2)))
    tile_peers = [(chip, c, j) for chip, j in tile_chips for c in range(2)] + [(ctx, other, colour)]
    sources = [chip_at(o, -1) for o in SHIFTS]
    for chip, c, _ in tile_peers:
        greet(chip, c)
    for offset in NEAR:
        for c in range(2):
            greet(chip_at(offset), c)

    loads[0].wait()
    chunk = 64

    @pl.loop(0, dspan // chunk)
    def _(i):
        rows = wq_s[pl.ds(i * chunk, chunk)].astype(F32).reshape(chunk * 8, 128)
        wq_f[pl.ds(pl.multiple_of(i * chunk * 8, 8), chunk * 8), :] = rows

    loads[1].wait()
    loads[2].wait()
    hid = hid_s[...].astype(F32).reshape(16, dspan).astype(BF16)
    for h in range(8):
        w_h = wq_f[pl.ds(h, dspan, stride=8), :].astype(BF16)
        qp[0, pl.ds(h, 16, stride=8), :] = jnp.dot(hid, w_h, preferred_element_type=F32)
    part_r = lax.dot_general(hid, wr_s[...].reshape(512, dspan), NT, preferred_element_type=F32)
    for pair in range(4):
        both = part_r[:, pair * 128:(pair + 1) * 128]
        qp[1, pl.ds(2 * pair, 16, stride=8), :] = both
        qp[1, pl.ds(2 * pair + 1, 16, stride=8), :] = pltpu.roll(both, 64, 1)
    loads[4].wait()
    for b in range(16):
        rope_p[b] = jnp.concatenate([rope_s[b, 0:32, :], rope_s[b, 32:64, :]], axis=1)
    loads[3].wait()

    pl.semaphore_wait(barrier, 39)
    for offset in RELAY:
        pl.semaphore_signal(near_sem, inc=1, device_id=dev(chip_at(offset), core), device_id_type=pl.DeviceIdType.MESH)

    def pair_rows(c):
        return pl.ds(pl.multiple_of(c * 16, 16), 16)

    for chip, peer in tile_chips:
        remote(qp.at[:, pair_rows(peer), :], rs1.at[colour], 0, dev(chip, core)).start()

    def cache_send(t, c, late):
        chip = chip_at(SHIFTS[t])
        target = (colour + STEPS[t][0]) % 4 + 4 * ((colour // 4 + STEPS[t][1]) % 2)
        src_row = 2 * target + c
        slot = 2 * t + core
        remote(lat_s.at[src_row], lat_b.at[slot], 12 if late else 1, dev(chip, c)).start()
        remote(rope_p.at[src_row], rope_b.at[slot], 13 if late else 2, dev(chip, c)).start()

    for t in (5, 6, 7):
        for c in range(2):
            cache_send(t, c, False)
    cache_send(0, other, False)
    own_l = pltpu.make_async_copy(lat_s.at[row], lat_b.at[core], own_sem.at[0])
    own_r = pltpu.make_async_copy(rope_p.at[row], rope_b.at[core], own_sem.at[1])
    own_l.start()
    own_r.start()
    rs1[colour] = qp[:, pair_rows(colour), :]

    for i in (6, 7, 8, 9):
        loads[i].start()
    loads[5].wait()
    arrived(rs1.at[pl.ds(0, 7)], 0)
    total = rs1[0]
    for i in range(1, 8):
        total = total + rs1[i]
    q_nope = total[0].astype(BF16)
    q_rope = jnp.where(lax.broadcasted_iota(jnp.int32, (16, 128), 1) < 64, total[1], 0.0)
    row_head = lax.broadcasted_iota(jnp.int32, (16, 512), 0) % 8
    q_lat = jnp.zeros((16, 512), F32)
    for h in range(8):
        res = jnp.dot(q_nope, wuk_s[h], preferred_element_type=F32)
        q_lat = jnp.where(row_head == h, res, q_lat)
    for r in range(2):
        q_send[r, :, 0:512] = q_lat[r * 8:(r + 1) * 8].astype(BF16)
        q_send[r, :, 512:640] = q_rope[r * 8:(r + 1) * 8].astype(BF16)
    pl.semaphore_wait(near_sem, 6)
    for chip, c, _ in class_peers:
        remote(q_send.at[c], q_all.at[me_class], 3, dev(chip, c)).start()
    for t in range(1, 5):
        for c in range(2):
            cache_send(t, c, True)
    q_all[me_class] = q_send[core]

    loads[8].wait()
    loads[9].wait()
    length = len_s[row]
    sub = lax.broadcasted_iota(jnp.int32, (8, dspan), 0)
    resid = jnp.zeros((8, dspan), F32)
    for i in range(8):
        block = hid_r[:, i * dspan:(i + 1) * dspan].astype(F32)
        line = jnp.sum(jnp.where(sub == row % 8, block, 0.0), axis=0, keepdims=True)
        resid = jnp.where(sub == i, line, resid)
    loads[6].wait()
    loads[7].wait()

    own_l.wait()
    own_r.wait()
    arrived(q_all.at[pl.ds(0, 15)], 3)
    arrived(lat_b.at[pl.ds(0, 7)], 1)
    arrived(rope_b.at[pl.ds(0, 7)], 2)
    queries = q_all[...].astype(F32).reshape(128, 640).astype(BF16)
    lane = lax.broadcasted_iota(jnp.int32, (128, 128), 1)

    def scores(t):
        keys = lat_b[2 * t:2 * t + 2].reshape(128, 512)
        packed = rope_b[2 * t:2 * t + 2]
        rkeys = jnp.concatenate([packed[:, :, 0:64], packed[:, :, 64:128]], axis=1).reshape(128, 64)
        s = lax.dot_general(queries[:, 0:512], keys, NT, preferred_element_type=F32)
        s = (s + lax.dot_general(queries[:, 512:576], rkeys, NT, preferred_element_type=F32)) * scale
        s = jnp.where(sources[t] * 128 + lane < length, s, NEG_FILL)
        s_buf[:, t * 128:(t + 1) * 128] = s
        return jnp.max(s, axis=1, keepdims=True)

    top = functools.reduce(jnp.maximum, [scores(t) for t in (0, 5, 6, 7)])
    arrived(lat_b.at[pl.ds(0, 8)], 12)
    arrived(rope_b.at[pl.ds(0, 8)], 13)
    top = functools.reduce(jnp.maximum, [top] + [scores(t) for t in range(1, 5)])
    den = jnp.zeros((128, 1), F32)
    for t in range(8):
        valid = sources[t] * 128 + lane < length
        w = jnp.where(valid, jnp.exp(s_buf[:, t * 128:(t + 1) * 128] - top), 0.0)
        den = den + jnp.sum(w, axis=1, keepdims=True)
        p_buf[:, t * 128:(t + 1) * 128] = w.astype(BF16)
    ml_send[...] = jnp.where(lane == 0, top, den).T[0:2]
    acc = jnp.dot(p_buf[...], lat_b[...].reshape(1024, 512), preferred_element_type=F32)
    acc_send[...] = acc.reshape(16, 8, 512)

    for chip, c, _ in class_peers:
        remote(ml_send, ml_all.at[me_class], 5, dev(chip, c)).start()
    for chip, c, peer in class_peers:
        remote(acc_send.at[peer], o_buf.at[me_class], 4, dev(chip, c)).start()
    o_buf[me_class] = acc_send[me_class]
    ml_all[me_class] = ml_send[...]
    arrived(ml_all.at[pl.ds(0, 15)], 5)
    ml_t[:, 0:32] = ml_all[...].reshape(32, 128).T
    ml = ml_t[pl.ds(pl.multiple_of(me_class * 8, 8), 8), :]
    factors, dens = [], []
    for r in range(2):
        m_all = [ml[:, 2 * (r * 8 + g):2 * (r * 8 + g) + 1] for g in range(8)]
        best = functools.reduce(jnp.maximum, m_all)
        den_r = jnp.zeros((8, 1), F32)
        for g in range(8):
            factor = jnp.exp(m_all[g] - best)
            den_r = den_r + ml[:, 2 * (r * 8 + g) + 1:2 * (r * 8 + g) + 2] * factor
            factors.append(jnp.broadcast_to(factor, (8, 512)))
        dens.append(den_r)
    arrived(o_buf.at[pl.ds(0, 15)], 4)
    finished = []
    for r in range(2):
        num = jnp.zeros((8, 512), F32)
        for g in range(8):
            num = num + o_buf[r * 8 + g] * factors[r * 8 + g]
        finished.append(num / dens[r])
    o_lat = jnp.concatenate(finished, axis=0).astype(BF16)
    row_head = lax.broadcasted_iota(jnp.int32, (16, 128), 0) % 8
    vals = jnp.zeros((16, 128), F32)
    for h in range(8):
        res = jnp.dot(o_lat, wuv_s[h], preferred_element_type=F32)
        vals = jnp.where(row_head == h, res, vals)

    spread = jnp.concatenate([jnp.where(row_head == h, vals, 0.0) for h in range(8)], axis=1).astype(BF16)

    def y_chunk(part, start, phase, sib):
        size = part.shape[2]
        piece_of = lax.broadcasted_iota(jnp.int32, (8, size), 0)
        sums = [jnp.zeros((8, size), F32), jnp.zeros((8, size), F32)]
        for i in range(0, 8, 2):
            cut = jnp.concatenate([wout_s[:, :, k * dspan + start:k * dspan + start + size].reshape(1024, size)
                                   for k in (i, i + 1)], axis=1)
            mixed = jnp.dot(spread, cut, preferred_element_type=F32)
            for k in range(2):
                for r in range(2):
                    line = jnp.sum(mixed[r * 8:(r + 1) * 8, k * size:(k + 1) * size], axis=0, keepdims=True)
                    sums[r] = jnp.where(piece_of == i + k, line, sums[r])
        part[0] = sums[0]
        part[1] = sums[1]
        remote(part.at[other], sib, phase, dev(ctx, other)).start()

    def y_share(part, sib, ysend, yall, swap_phase, phase):
        arrived(sib, swap_phase)
        ysend[...] = part[core] + sib[...]
        for chip, _ in class_chips:
            remote(ysend, yall.at[group], phase, dev(chip, core)).start()
        yall[group] = ysend[...]

    def out_share(yall, piece, dest, start, y_phase, phase):
        arrived(yall.at[pl.ds(0, 7)], y_phase)
        y_sum = yall[0]
        for g in range(1, 8):
            y_sum = y_sum + yall[g]
        piece[...] = (resid[:, start:start + piece.shape[1]] + y_sum).astype(BF16)
        for chip, c, _ in tile_peers:
            remote(piece, dest.at[me_tile], phase, dev(chip, c)).start()
        dest[me_tile] = piece[...]

    first = part_a.shape[2]
    y_chunk(part_a, 0, 6, sib_a)
    y_chunk(part_b, first, 7, sib_b)
    y_share(part_a, sib_a, ysend_a, yall_a, 6, 8)
    y_share(part_b, sib_b, ysend_b, yall_b, 7, 9)
    out_share(yall_a, piece_a, out_a, 0, 8, 10)
    out_share(yall_b, piece_b, out_b, first, 9, 11)

    def place(pieces, start):
        for tile in range(pieces.shape[2] // 128):
            rows_f[...] = pieces[:, :, tile * 128:(tile + 1) * 128].astype(F32).reshape(128, 128)
            for i in range(8):
                lanes = pl.ds(i * dspan + start + tile * 128, 128)
                rows = rows_f[pl.ds(i, 16, stride=8), :]
                out[0, :, lanes] = rows[0:8].astype(BF16)
                out[1, :, lanes] = rows[8:16].astype(BF16)

    arrived(out_a.at[pl.ds(0, 15)], 10)
    place(out_a, 0)
    arrived(out_b.at[pl.ds(0, 15)], 11)
    place(out_b, first)
    left(rs1.at[pl.ds(0, 7)], 0)
    left(lat_b.at[pl.ds(0, 7)], 1)
    left(rope_b.at[pl.ds(0, 7)], 2)
    left(lat_b.at[pl.ds(0, 8)], 12)
    left(rope_b.at[pl.ds(0, 8)], 13)
    left(q_all.at[pl.ds(0, 15)], 3)
    left(o_buf.at[pl.ds(0, 15)], 4)
    left(ml_all.at[pl.ds(0, 15)], 5)
    left(sib_a, 6)
    left(sib_b, 7)
    left(yall_a.at[pl.ds(0, 7)], 8)
    left(yall_b.at[pl.ds(0, 7)], 9)
    left(out_a.at[pl.ds(0, 15)], 10)
    left(out_b.at[pl.ds(0, 15)], 11)


def finish(rows, out, sem):
    copy = pltpu.make_async_copy(rows, out, sem)
    copy.start()
    copy.wait()


def solution(mesh):
    row_spec = P('batch', None)
    cache_spec = P('batch', ('ctx', 'seq'), None)
    proj_spec = P(None, 'seq', None)
    head_spec = P('seq', None, None)

    def local_step(hidden, lengths, latent_cache, rope_keys, w_uq, w_qr, w_uk, w_uv, w_out):
        scale = (w_uq.shape[2] + w_qr.shape[2]) ** -0.5
        width = hidden.shape[1]
        dspan = width // 8
        first = dspan // 128 // 2 * 128 + 128
        second = dspan - first
        vmem, dma = pltpu.VMEM, pltpu.SemaphoreType.DMA
        anywhere = pl.BlockSpec(memory_space=pl.ANY)
        scratch = [
            pltpu.SMEM((16,), jnp.int32),
            vmem((2, 8, dspan), BF16),
            vmem((8, width), BF16),
            vmem((dspan, 8, 128), BF16),
            vmem((dspan * 8, 128), F32),
            vmem((8, 64, dspan), BF16),
            vmem((8, 128, 512), BF16),
            vmem((8, 512, 128), BF16),
            vmem((8, 128, width), BF16),
            vmem((16, 64, 512), BF16),
            vmem((16, 64, 64), BF16),
            vmem((16, 32, 128), BF16),
            vmem((16, 64, 512), BF16),
            vmem((16, 32, 128), BF16),
            vmem((2, 128, 128), F32),
            vmem((8, 2, 16, 128), F32),
            vmem((2, 8, 640), BF16),
            vmem((16, 8, 640), BF16),
            vmem((128, 1024), F32),
            vmem((128, 1024), BF16),
            vmem((16, 8, 512), F32),
            vmem((16, 8, 512), F32),
            vmem((2, 128), F32),
            vmem((16, 2, 128), F32),
            vmem((128, 128), F32),
            vmem((2, 8, first), F32),
            vmem((2, 8, second), F32),
            vmem((8, first), F32),
            vmem((8, second), F32),
            vmem((8, first), F32),
            vmem((8, second), F32),
            vmem((8, 8, first), F32),
            vmem((8, 8, second), F32),
            vmem((8, first), BF16),
            vmem((8, second), BF16),
            vmem((16, 8, first), BF16),
            vmem((16, 8, second), BF16),
            vmem((128, 128), F32),
            dma((10,)), dma((2,)), dma((14,)), dma((14,)), pltpu.SemaphoreType.REGULAR,
        ]
        out = pl.pallas_call(
            functools.partial(kernel, scale),
            out_shape=vmem((2, 8, width), BF16),
            in_specs=[anywhere] * 9,
            out_specs=pl.BlockSpec(memory_space=pltpu.VMEM),
            scratch_shapes=scratch,
            compiler_params=pltpu.CompilerParams(collective_id=0, has_side_effects=True,
                                                 vmem_limit_bytes=60 * 1024 * 1024),
            name='mla_decode',
        )(hidden.reshape(2, 8, width), lengths, latent_cache, rope_keys, w_uq,
          jnp.transpose(w_qr, (1, 2, 0)), w_uk, w_uv, w_out)
        done = pl.pallas_call(
            finish,
            out_shape=jax.ShapeDtypeStruct((2, 8, width), BF16),
            in_specs=[pl.BlockSpec(memory_space=pltpu.VMEM)],
            out_specs=pl.BlockSpec(memory_space=pl.ANY),
            scratch_shapes=[dma],
            name='mla_out',
        )(pltpu.with_memory_space_constraint(out, pltpu.VMEM))
        return done.reshape(16, width)

    return jax.shard_map(local_step, mesh=mesh,
                         in_specs=(row_spec, P('batch'), cache_spec, cache_spec, proj_spec, proj_spec, head_spec, head_spec, head_spec),
                         out_specs=row_spec, check_vma=False)
```

```python
import functools

import jax
import jax.numpy as jnp
from jax import lax
from jax.experimental import pallas as pl
from jax.experimental.pallas import tpu as pltpu
from jax.sharding import PartitionSpec as P

NEG_FILL = -1.0e30
F32 = jnp.float32
BF16 = jnp.bfloat16

SHIFTS = ((0, 0, 0), (1, 0, 0), (0, 0, -1), (0, 1, 0), (0, -1, 0), (-1, 0, -1), (1, -1, 0), (0, 1, 1))
STEPS = ((0, 0), (1, 0), (3, 0), (1, 1), (3, 1), (2, 0), (0, 1), (2, 1))

LANES, LATENT, ROWS, OCT, HALF, WIDE, QWIDE, HALVED, PEERS, CHIPS = 128, 512, 16, 8, 64, 1024, 640, 32, 15, 7
NT = (((1,), (1,)), ((), ()))


CLASS = ((2, 2, 0), (0, 2, 2), (2, 0, 2), (1, 2, 1), (3, 2, 3), (1, 0, 3), (3, 0, 1))
NEAR = ((0, 1, 0), (0, 3, 0), (0, 0, 1), (0, 0, 3), (1, 0, 1), (3, 0, 3), (1, 3, 0), (3, 1, 0), (0, 1, 1), (0, 3, 3),
        (1, 1, 0), (3, 3, 0))
RELAY = ((0, 1, 1), (0, 3, 3), (1, 0, 1), (1, 3, 0), (1, 0, 0), (3, 0, 0))


def kernel(scale, hidden, lengths, latent, rope, wuq, wqr, wuk, wuv, wout, out,
           len_s, hid_s, hid_r, wq_s, wq_f, wr_s, wuk_s, wuv_s, wout_s, lat_s, rope_s, rope_p,
           lat_b, rope_b, qp, rs1, q_send, q_all, s_buf, p_buf, acc_send, o_buf, ml_send, ml_all, ml_t,
           part_a, part_b, sib_a, sib_b, ysend_a, ysend_b, yall_a, yall_b, piece_a, piece_b, out_a, out_b, rows_f,
           load_sem, own_sem, send_sem, recv_sem, near_sem):
    ctx = lax.axis_index('ctx')
    core = lax.axis_index('seq')
    z, y, x = ctx // ROWS, (ctx // 4) % 4, ctx % 4
    xs = [(x + d) % 4 for d in range(4)]
    ys = [(y + d) % 4 for d in range(4)]
    zs = [(z + d) % 4 for d in range(4)]
    ys4 = [v * 4 for v in ys]
    zs16 = [v * ROWS for v in zs]

    def chip_at(offset, sign=1):
        dx, dy, dz = offset
        return zs16[sign * dz % 4] + ys4[sign * dy % 4] + xs[sign * dx % 4]

    colour = (x + y + z) % 4 + 4 * (y % 2)
    group = z * 2 + y // 2
    other = 1 - core
    row = 2 * colour + core
    dspan = hid_s.shape[2]
    cols = pl.ds(pl.multiple_of(colour * dspan, LANES), dspan)
    heads = pl.ds(pl.multiple_of(group * OCT, OCT), OCT)

    def dev(chip, c):
        return (0, chip, c)

    def remote(src, dst, phase, device):
        return pltpu.make_async_remote_copy(src_ref=src, dst_ref=dst, send_sem=send_sem.at[phase],
                                            recv_sem=recv_sem.at[phase], device_id=device,
                                            device_id_type=pl.DeviceIdType.MESH)

    def arrived(part, phase):
        remote(part, part, phase, dev(ctx, other)).wait_recv()

    def left(part, phase):
        remote(part, part, phase, dev(ctx, other)).wait_send()

    loads = [
        pltpu.make_async_copy(wuq.at[pl.ds(pl.multiple_of(colour * dspan, LANES), dspan), heads, :], wq_s, load_sem.at[0]),
        pltpu.make_async_copy(wqr.at[heads, :, cols], wr_s, load_sem.at[1]),
        pltpu.make_async_copy(hidden.at[:, :, cols], hid_s, load_sem.at[2]),
        pltpu.make_async_copy(latent, lat_s, load_sem.at[3]),
        pltpu.make_async_copy(rope, rope_s, load_sem.at[4]),
        pltpu.make_async_copy(wuk.at[heads], wuk_s, load_sem.at[5]),
        pltpu.make_async_copy(wuv.at[heads], wuv_s, load_sem.at[6]),
        pltpu.make_async_copy(wout.at[heads], wout_s, load_sem.at[CHIPS]),
        pltpu.make_async_copy(lengths, len_s, load_sem.at[OCT]),
        pltpu.make_async_copy(hidden.at[row // OCT], hid_r, load_sem.at[9]),
    ]
    for i in (0, 1, 2, 4, 3, 5):
        loads[i].start()

    barrier = pltpu.get_barrier_semaphore()

    def greet(chip, c):
        pl.semaphore_signal(barrier, inc=1, device_id=dev(chip, c), device_id_type=pl.DeviceIdType.MESH)

    me_class = core * OCT + group
    me_tile = colour * 2 + core
    class_chips = [(chip_at(o), zs[o[2]] * 2 + ys[o[1]] // 2) for o in CLASS]
    class_peers = [(chip, c, c * OCT + g) for chip, g in class_chips for c in range(2)] + [(ctx, other, other * OCT + group)]
    mate = y + 1 - 2 * (y % 2)
    tile_chips = []
    for d in (2, 1, 3):
        tile_chips.append((z * ROWS + mate * 4 + xs[d], (xs[d] + mate + z) % 4 + 4 * (mate % 2)))
    tile_chips.append((zs16[0] + ys4[0] + xs[2], (xs[2] + y + z) % 4 + 4 * (y % 2)))
    tile_chips.append((z * ROWS + mate * 4 + x, (x + mate + z) % 4 + 4 * (mate % 2)))
    for d in (1, 3):
        tile_chips.append((zs16[0] + ys4[0] + xs[d], (xs[d] + y + z) % 4 + 4 * (y % 2)))
    tile_peers = [(chip, c, j) for chip, j in tile_chips for c in range(2)] + [(ctx, other, colour)]
    sources = [chip_at(o, -1) for o in SHIFTS]
    for chip, c, _ in tile_peers:
        greet(chip, c)
    for offset in NEAR:
        for c in range(2):
            greet(chip_at(offset), c)

    loads[0].wait()
    chunk = HALF

    @pl.loop(0, dspan // chunk)
    def _(i):
        rows = wq_s[pl.ds(i * chunk, chunk)].astype(F32).reshape(chunk * OCT, LANES)
        wq_f[pl.ds(pl.multiple_of(i * chunk * OCT, OCT), chunk * OCT), :] = rows

    loads[1].wait()
    loads[2].wait()
    hid = hid_s[...].astype(F32).reshape(ROWS, dspan).astype(BF16)
    w_n = jnp.concatenate([wq_f[pl.ds(h, dspan, stride=OCT), :].astype(BF16) for h in range(OCT)], axis=1)
    part_n = jnp.dot(hid, w_n, preferred_element_type=F32)
    for h in range(OCT):
        qp[0, pl.ds(h, ROWS, stride=OCT), :] = part_n[:, h * LANES:(h + 1) * LANES]
    part_r = lax.dot_general(hid, wr_s[...].reshape(LATENT, dspan), NT, preferred_element_type=F32)
    for pair in range(4):
        both = part_r[:, pair * LANES:(pair + 1) * LANES]
        qp[1, pl.ds(2 * pair, ROWS, stride=OCT), :] = both
        qp[1, pl.ds(2 * pair + 1, ROWS, stride=OCT), :] = pltpu.roll(both, HALF, 1)
    loads[4].wait()
    for b in range(ROWS):
        rope_p[b] = jnp.concatenate([rope_s[b, 0:HALVED, :], rope_s[b, HALVED:HALF, :]], axis=1)
    loads[3].wait()

    pl.semaphore_wait(barrier, 39)
    for offset in RELAY:
        pl.semaphore_signal(near_sem, inc=1, device_id=dev(chip_at(offset), core), device_id_type=pl.DeviceIdType.MESH)

    def pair_rows(c):
        return pl.ds(pl.multiple_of(c * ROWS, ROWS), ROWS)

    for chip, peer in tile_chips:
        remote(qp.at[:, pair_rows(peer), :], rs1.at[colour], 0, dev(chip, core)).start()

    def cache_send(t, c, late):
        chip = chip_at(SHIFTS[t])
        target = (colour + STEPS[t][0]) % 4 + 4 * ((colour // 4 + STEPS[t][1]) % 2)
        src_row = 2 * target + c
        slot = 2 * t + core
        remote(lat_s.at[src_row], lat_b.at[slot], 12 if late else 1, dev(chip, c)).start()
        remote(rope_p.at[src_row], rope_b.at[slot], 13 if late else 2, dev(chip, c)).start()

    for t in (5, 6, CHIPS):
        for c in range(2):
            cache_send(t, c, False)
    cache_send(0, other, False)
    own_l = pltpu.make_async_copy(lat_s.at[row], lat_b.at[core], own_sem.at[0])
    own_r = pltpu.make_async_copy(rope_p.at[row], rope_b.at[core], own_sem.at[1])
    own_l.start()
    own_r.start()
    rs1[colour] = qp[:, pair_rows(colour), :]

    for i in (6, CHIPS, OCT, 9):
        loads[i].start()
    loads[5].wait()
    arrived(rs1.at[pl.ds(0, CHIPS)], 0)
    total = rs1[0]
    for i in range(1, OCT):
        total = total + rs1[i]
    row_head = lax.broadcasted_iota(jnp.int32, (ROWS, LANES), 0) % OCT
    q_nope = jnp.concatenate([jnp.where(row_head == h, total[0], 0.0) for h in range(OCT)], axis=1).astype(BF16)
    q_rope = jnp.where(lax.broadcasted_iota(jnp.int32, (ROWS, LANES), 1) < HALF, total[1], 0.0)
    q_lat = jnp.dot(q_nope, wuk_s[...].reshape(WIDE, LATENT), preferred_element_type=F32)
    for r in range(2):
        q_send[r, :, 0:LATENT] = q_lat[r * OCT:(r + 1) * OCT].astype(BF16)
        q_send[r, :, LATENT:QWIDE] = q_rope[r * OCT:(r + 1) * OCT].astype(BF16)
    pl.semaphore_wait(near_sem, 6)
    for chip, c, _ in class_peers:
        remote(q_send.at[c], q_all.at[me_class], 3, dev(chip, c)).start()
    for t in range(1, 5):
        for c in range(2):
            cache_send(t, c, True)
    q_all[me_class] = q_send[core]

    loads[OCT].wait()
    loads[9].wait()
    length = len_s[row]
    sub = lax.broadcasted_iota(jnp.int32, (OCT, dspan), 0)
    resid = jnp.zeros((OCT, dspan), F32)
    for i in range(OCT):
        block = hid_r[:, i * dspan:(i + 1) * dspan].astype(F32)
        line = jnp.sum(jnp.where(sub == row % OCT, block, 0.0), axis=0, keepdims=True)
        resid = jnp.where(sub == i, line, resid)
    loads[6].wait()
    loads[CHIPS].wait()

    own_l.wait()
    own_r.wait()
    arrived(q_all.at[pl.ds(0, PEERS)], 3)
    arrived(lat_b.at[pl.ds(0, CHIPS)], 1)
    arrived(rope_b.at[pl.ds(0, CHIPS)], 2)
    queries = q_all[...].astype(F32).reshape(LANES, QWIDE).astype(BF16)
    lane = lax.broadcasted_iota(jnp.int32, (LANES, LANES), 1)

    def scores(t):
        keys = lat_b[2 * t:2 * t + 2].reshape(LANES, LATENT)
        packed = rope_b[2 * t:2 * t + 2]
        rkeys = jnp.concatenate([packed[:, :, 0:HALF], packed[:, :, HALF:LANES]], axis=1).reshape(LANES, HALF)
        s = lax.dot_general(queries[:, 0:LATENT], keys, NT, preferred_element_type=F32)
        s = (s + lax.dot_general(queries[:, LATENT:576], rkeys, NT, preferred_element_type=F32)) * scale
        s = jnp.where(sources[t] * LANES + lane < length, s, NEG_FILL)
        s_buf[:, t * LANES:(t + 1) * LANES] = s
        return jnp.max(s, axis=1, keepdims=True)

    top = functools.reduce(jnp.maximum, [scores(t) for t in (0, 5, 6, CHIPS)])
    arrived(lat_b.at[pl.ds(0, OCT)], 12)
    arrived(rope_b.at[pl.ds(0, OCT)], 13)
    top = functools.reduce(jnp.maximum, [top] + [scores(t) for t in range(1, 5)])
    den = jnp.zeros((LANES, 1), F32)
    for t in range(OCT):
        valid = sources[t] * LANES + lane < length
        w = jnp.where(valid, jnp.exp(s_buf[:, t * LANES:(t + 1) * LANES] - top), 0.0)
        den = den + jnp.sum(w, axis=1, keepdims=True)
        p_buf[:, t * LANES:(t + 1) * LANES] = w.astype(BF16)
    ml_send[...] = jnp.where(lane == 0, top, den).T[0:2]
    acc = jnp.dot(p_buf[...], lat_b[...].reshape(WIDE, LATENT), preferred_element_type=F32)
    acc_send[...] = acc.reshape(ROWS, OCT, LATENT)

    for chip, c, _ in class_peers:
        remote(ml_send, ml_all.at[me_class], 5, dev(chip, c)).start()
    for chip, c, peer in class_peers:
        remote(acc_send.at[peer], o_buf.at[me_class], 4, dev(chip, c)).start()
    o_buf[me_class] = acc_send[me_class]
    ml_all[me_class] = ml_send[...]
    arrived(ml_all.at[pl.ds(0, PEERS)], 5)
    ml_t[:, 0:HALVED] = ml_all[...].reshape(HALVED, LANES).T
    ml = ml_t[pl.ds(pl.multiple_of(me_class * OCT, OCT), OCT), :]
    factors, dens = [], []
    for r in range(2):
        m_all = [ml[:, 2 * (r * OCT + g):2 * (r * OCT + g) + 1] for g in range(OCT)]
        best = functools.reduce(jnp.maximum, m_all)
        den_r = jnp.zeros((OCT, 1), F32)
        for g in range(OCT):
            factor = jnp.exp(m_all[g] - best)
            den_r = den_r + ml[:, 2 * (r * OCT + g) + 1:2 * (r * OCT + g) + 2] * factor
            factors.append(jnp.broadcast_to(factor, (OCT, LATENT)))
        dens.append(den_r)
    arrived(o_buf.at[pl.ds(0, PEERS)], 4)
    finished = []
    for r in range(2):
        num = jnp.zeros((OCT, LATENT), F32)
        for g in range(OCT):
            num = num + o_buf[r * OCT + g] * factors[r * OCT + g]
        finished.append(num / dens[r])
    o_lat = jnp.concatenate(finished, axis=0).astype(BF16)
    w_v = jnp.concatenate([wuv_s[h] for h in range(OCT)], axis=1)
    every = jnp.dot(o_lat, w_v, preferred_element_type=F32)
    vals = jnp.zeros((ROWS, LANES), F32)
    for h in range(OCT):
        vals = jnp.where(row_head == h, every[:, h * LANES:(h + 1) * LANES], vals)

    spread = jnp.concatenate([jnp.where(row_head == h, vals, 0.0) for h in range(OCT)], axis=1).astype(BF16)

    def y_chunk(part, start, phase, sib):
        size = part.shape[2]
        piece_of = lax.broadcasted_iota(jnp.int32, (OCT, size), 0)
        sums = [jnp.zeros((OCT, size), F32), jnp.zeros((OCT, size), F32)]
        for i in range(0, OCT, 2):
            cut = jnp.concatenate([wout_s[:, :, k * dspan + start:k * dspan + start + size].reshape(WIDE, size)
                                   for k in (i, i + 1)], axis=1)
            mixed = jnp.dot(spread, cut, preferred_element_type=F32)
            for k in range(2):
                for r in range(2):
                    line = jnp.sum(mixed[r * OCT:(r + 1) * OCT, k * size:(k + 1) * size], axis=0, keepdims=True)
                    sums[r] = jnp.where(piece_of == i + k, line, sums[r])
        part[0] = sums[0]
        part[1] = sums[1]
        remote(part.at[other], sib, phase, dev(ctx, other)).start()

    def y_share(part, sib, ysend, yall, swap_phase, phase):
        arrived(sib, swap_phase)
        ysend[...] = part[core] + sib[...]
        for chip, _ in class_chips:
            remote(ysend, yall.at[group], phase, dev(chip, core)).start()
        yall[group] = ysend[...]

    def out_share(yall, piece, dest, start, y_phase, phase):
        arrived(yall.at[pl.ds(0, CHIPS)], y_phase)
        y_sum = yall[0]
        for g in range(1, OCT):
            y_sum = y_sum + yall[g]
        piece[...] = (resid[:, start:start + piece.shape[1]] + y_sum).astype(BF16)
        for chip, c, _ in tile_peers:
            remote(piece, dest.at[me_tile], phase, dev(chip, c)).start()
        dest[me_tile] = piece[...]

    first = part_a.shape[2]
    y_chunk(part_a, 0, 6, sib_a)
    y_chunk(part_b, first, CHIPS, sib_b)
    y_share(part_a, sib_a, ysend_a, yall_a, 6, OCT)
    y_share(part_b, sib_b, ysend_b, yall_b, CHIPS, 9)
    out_share(yall_a, piece_a, out_a, 0, OCT, 10)
    out_share(yall_b, piece_b, out_b, first, 9, 11)

    def place(pieces, start):
        for tile in range(pieces.shape[2] // LANES):
            rows_f[...] = pieces[:, :, tile * LANES:(tile + 1) * LANES].astype(F32).reshape(LANES, LANES)
            for i in range(OCT):
                lanes = pl.ds(i * dspan + start + tile * LANES, LANES)
                rows = rows_f[pl.ds(i, ROWS, stride=OCT), :]
                out[0, :, lanes] = rows[0:OCT].astype(BF16)
                out[1, :, lanes] = rows[OCT:ROWS].astype(BF16)

    arrived(out_a.at[pl.ds(0, PEERS)], 10)
    place(out_a, 0)
    arrived(out_b.at[pl.ds(0, PEERS)], 11)
    place(out_b, first)
    left(rs1.at[pl.ds(0, CHIPS)], 0)
    left(lat_b.at[pl.ds(0, CHIPS)], 1)
    left(rope_b.at[pl.ds(0, CHIPS)], 2)
    left(lat_b.at[pl.ds(0, OCT)], 12)
    left(rope_b.at[pl.ds(0, OCT)], 13)
    left(q_all.at[pl.ds(0, PEERS)], 3)
    left(o_buf.at[pl.ds(0, PEERS)], 4)
    left(ml_all.at[pl.ds(0, PEERS)], 5)
    left(sib_a, 6)
    left(sib_b, CHIPS)
    left(yall_a.at[pl.ds(0, CHIPS)], OCT)
    left(yall_b.at[pl.ds(0, CHIPS)], 9)
    left(out_a.at[pl.ds(0, PEERS)], 10)
    left(out_b.at[pl.ds(0, PEERS)], 11)


def finish(rows, out, sem):
    copy = pltpu.make_async_copy(rows, out, sem)
    copy.start()
    copy.wait()


def solution(mesh):
    row_spec = P('batch', None)
    cache_spec = P('batch', ('ctx', 'seq'), None)
    proj_spec = P(None, 'seq', None)
    head_spec = P('seq', None, None)

    def local_step(hidden, lengths, latent_cache, rope_keys, w_uq, w_qr, w_uk, w_uv, w_out):
        scale = (w_uq.shape[2] + w_qr.shape[2]) ** -0.5
        width = hidden.shape[1]
        dspan = width // OCT
        first = dspan // LANES // 2 * LANES + LANES
        second = dspan - first
        vmem, dma = pltpu.VMEM, pltpu.SemaphoreType.DMA
        anywhere = pl.BlockSpec(memory_space=pl.ANY)
        scratch = [
            pltpu.SMEM((ROWS,), jnp.int32),
            vmem((2, OCT, dspan), BF16),
            vmem((OCT, width), BF16),
            vmem((dspan, OCT, LANES), BF16),
            vmem((dspan * OCT, LANES), F32),
            vmem((OCT, HALF, dspan), BF16),
            vmem((OCT, LANES, LATENT), BF16),
            vmem((OCT, LATENT, LANES), BF16),
            vmem((OCT, LANES, width), BF16),
            vmem((ROWS, HALF, LATENT), BF16),
            vmem((ROWS, HALF, HALF), BF16),
            vmem((ROWS, HALVED, LANES), BF16),
            vmem((ROWS, HALF, LATENT), BF16),
            vmem((ROWS, HALVED, LANES), BF16),
            vmem((2, LANES, LANES), F32),
            vmem((OCT, 2, ROWS, LANES), F32),
            vmem((2, OCT, QWIDE), BF16),
            vmem((ROWS, OCT, QWIDE), BF16),
            vmem((LANES, WIDE), F32),
            vmem((LANES, WIDE), BF16),
            vmem((ROWS, OCT, LATENT), F32),
            vmem((ROWS, OCT, LATENT), F32),
            vmem((2, LANES), F32),
            vmem((ROWS, 2, LANES), F32),
            vmem((LANES, LANES), F32),
            vmem((2, OCT, first), F32),
            vmem((2, OCT, second), F32),
            vmem((OCT, first), F32),
            vmem((OCT, second), F32),
            vmem((OCT, first), F32),
            vmem((OCT, second), F32),
            vmem((OCT, OCT, first), F32),
            vmem((OCT, OCT, second), F32),
            vmem((OCT, first), BF16),
            vmem((OCT, second), BF16),
            vmem((ROWS, OCT, first), BF16),
            vmem((ROWS, OCT, second), BF16),
            vmem((LANES, LANES), F32),
            dma((10,)), dma((2,)), dma((14,)), dma((14,)), pltpu.SemaphoreType.REGULAR,
        ]
        out = pl.pallas_call(
            functools.partial(kernel, scale),
            out_shape=vmem((2, OCT, width), BF16),
            in_specs=[anywhere] * 9,
            out_specs=pl.BlockSpec(memory_space=pltpu.VMEM),
            scratch_shapes=scratch,
            compiler_params=pltpu.CompilerParams(collective_id=0, has_side_effects=True,
                                                 vmem_limit_bytes=60 * WIDE * WIDE),
            name='mla_decode',
        )(hidden.reshape(2, OCT, width), lengths, latent_cache, rope_keys, w_uq,
          jnp.transpose(w_qr, (1, 2, 0)), w_uk, w_uv, w_out)
        done = pl.pallas_call(
            finish,
            out_shape=jax.ShapeDtypeStruct((2, OCT, width), BF16),
            in_specs=[pl.BlockSpec(memory_space=pltpu.VMEM)],
            out_specs=pl.BlockSpec(memory_space=pl.ANY),
            scratch_shapes=[dma],
            name='mla_out',
        )(pltpu.with_memory_space_constraint(out, pltpu.VMEM))
        return done.reshape(ROWS, width)

    return jax.shard_map(local_step, mesh=mesh,
                         in_specs=(row_spec, P('batch'), cache_spec, cache_spec, proj_spec, proj_spec, head_spec, head_spec, head_spec),
                         out_specs=row_spec, check_vma=False)
```
